256 devices in a mesh: groups: 2 (over y), seq: 2 (over core), row: 16 (over z), col: 4 (over x).
Axes of the slice: x: 4, y: 2, z: 16, core: 2. Of those that a mesh axis runs over, the one named last changes fastest.
The devices are a block of a 4x16x16 slice.
Arguments:
- paired_left: bfloat16 [1024, 32, 512], P(('groups', 'seq', 'col'), None, 'row'), parts along dimension 0, may hold values from -24 to 24
- paired_right: bfloat16 [1024, 32, 512], P(('groups', 'seq', 'row'), None, 'col'), parts along dimension 0, may hold values from -24 to 24
- unpaired_left: bfloat16 [2048, 32, 512], P(('groups', 'seq', 'col'), None, 'row'), parts along dimension 0, may hold values from -24 to 24
- unpaired_right: bfloat16 [2048, 32, 512], P(('groups', 'seq', 'row'), None, 'col'), parts along dimension 0, may hold values from -24 to 24
- out_weight: bfloat16 [1024, 128], replicated, may hold values from -0.1875 to 0.1875
- out_bias: float32 [128], replicated, may hold values from -6 to 6
- chain_lengths: int32 [24], P('groups'), parts along dimension 0, may hold values from 1 to 128, 512 in all
- unpaired_depths: int32 [24], P('groups'), parts along dimension 0, may hold values from 256 to 1024
Outputs:
- pair_update: bfloat16 [1024, 512, 128], P(('groups', 'row'), ('col', 'seq')), parts along dimension 0
The draws below stay inside these ranges and needn't reach their ends.
There are 2 independent parts, one for each index of `groups`. The reference program is written for one: setup_inputs(seed, part) draws one part's arguments, and reference() takes and returns one part's arrays. A program takes and returns all parts, laid end to end along the dimension named above; an argument that names none is the same for every part. Nothing has to cross between parts.
Inputs may be any that keep to these rules, and one draw needn't show every extreme that they name: `chain_lengths`: chain lengths sum to 512. `unpaired_depths`: rows of the unpaired MSA at or beyond a chain's depth are padding.
All inputs are finite; a program needn't handle non-finite values.
Results may differ from the reference program's by a relative error of at most 0.0034.
Values may be sent and summed in bfloat16 or wider, within the bound.
No kernel may reach another device: no remote copies, remote signals or barrier semaphores. Data moves between devices by JAX's collectives and lax.ppermute only.
A program may use at most 64 MiB of HBM per device.

```python
import math
import jax
import jax.numpy as jnp
import numpy as np
from jax import lax

C = 32
Z = 128
CHAINS = 12
S_P = 512
DMAX = 1024
N = 512
N_SEQ = 2


def place_ends(result, own_key, least, top_value):
    longest = result.shape.index(max(result.shape))
    spots = []
    for shift in (0, 1):
        where = [jax.random.randint(jax.random.fold_in(own_key, axis), (), 0, length) for axis, length in enumerate(result.shape)]
        where[longest] = (where[longest] + shift) % result.shape[longest]
        spots.append(tuple(where))
    return result.at[spots[0]].set(least).at[spots[1]].set(top_value)


def block_scale(key, shape, shards, least, high):
    level = 1.0
    for axis_at, parts in shards:
        steps = jax.random.uniform(jax.random.fold_in(jax.random.fold_in(key, 6), axis_at), (parts,), jnp.float32, least / len(shards), high / len(shards))
        level = level * jnp.repeat(jnp.exp(steps), shape[axis_at] // parts).reshape((-1,) + (1,) * (len(shape) - 1 - axis_at))
    return level


def length_profile(number_of, total, bound, skew):
    weights = [(1 << 20) // math.isqrt(rank ** skew) + 1 for rank in range(2, number_of + 1)]
    spare, given = total - bound - (number_of - 1), [1] * (number_of - 1)
    while spare > 0:
        free = [i for i in range(number_of - 1) if given[i] < bound]
        pool, left = sum([weights[i] for i in free]), spare
        for i in free:
            more = min(bound - given[i], max(1, left * weights[i] // pool), spare)
            given[i] = given[i] + more
            spare = spare - more
    return np.array([bound] + given)


def ragged_sizes(key, number_of, total, most, lean):
    if number_of == 2:
        one = jax.random.randint(key, (), max(1, total - most), min(most, total - 1) + 1)
        return jnp.stack([one, total - one])
    sizes = jnp.asarray(length_profile(number_of, total, most, lean), jnp.int32)
    couples = (number_of - 1) // 2
    source_of, taker = sizes[1:1 + 2 * couples:2], sizes[2:2 + 2 * couples:2]
    slack = jnp.minimum(source_of - 1, most - taker)
    moved = jax.random.randint(jax.random.fold_in(key, 1), (couples,), 0, 1 << 20) % (slack + 1)
    sizes = sizes.at[1:1 + 2 * couples:2].set(source_of - moved).at[2:2 + 2 * couples:2].set(taker + moved)
    return sizes[jax.random.permutation(jax.random.fold_in(key, 2), number_of)]


def scatter_about(own_key, shape, spread, bound, split=(), kind=jnp.bfloat16):
    factor_of = block_scale(own_key, shape, split, -0.22, 0.18) if split else 1.0
    values = jax.random.normal(own_key, shape, jnp.float32) * spread * factor_of
    return jnp.minimum(jnp.maximum(values, -bound), bound).astype(kind)


def setup_inputs(seed: int = 0, part: int = 0) -> dict:
    streams_of = jax.random.split(jax.random.key(seed), 9)
    part_keys = jax.random.split(jax.random.fold_in(streams_of[8], part), 9)
    paired_left = scatter_about(part_keys[0], (S_P, C, N), 4.0, 24.0, ((0, 8), (2, 16)))
    paired_right = scatter_about(part_keys[1], (S_P, C, N), 4.0, 24.0, ((0, 32), (2, 4)))
    unpaired_left = scatter_about(part_keys[2], (DMAX, C, N), 4.0, 24.0, ((0, 8), (2, 16)))
    unpaired_right = scatter_about(part_keys[3], (DMAX, C, N), 4.0, 24.0, ((0, 32), (2, 4)))
    out_weight = scatter_about(streams_of[4], (C * C, Z), (C * C) ** -0.5, 0.1875)
    out_bias = scatter_about(streams_of[5], (Z,), 1.0, 6.0, (), jnp.float32)
    chain_lengths = ragged_sizes(part_keys[6], CHAINS, N, N // 4, 1).astype(jnp.int32)
    unpaired_depths = place_ends(jax.random.randint(part_keys[7], (CHAINS,), DMAX // 4, DMAX + 1), jax.random.fold_in(part_keys[7], 1), DMAX // 4, DMAX).astype(jnp.int32)
    return {"paired_left": paired_left, "paired_right": paired_right, "unpaired_left": unpaired_left, "unpaired_right": unpaired_right, "out_weight": out_weight, "out_bias": out_bias, "chain_lengths": chain_lengths, "unpaired_depths": unpaired_depths}


def chain_tables(chain_lengths, unpaired_depths):
    positions = jnp.arange(N, dtype=jnp.int32)
    chain_ends = jnp.cumsum(chain_lengths).astype(jnp.int32)
    chain_of = jnp.sum((positions[:, None] >= chain_ends[None, :]).astype(jnp.int32), axis=1).astype(jnp.int32)
    onehot = chain_of[:, None] == jnp.arange(CHAINS, dtype=jnp.int32)[None, :]
    depth_of = jnp.sum(jnp.where(onehot, unpaired_depths[None, :], 0), axis=1).astype(jnp.int32)
    return chain_of, depth_of


def reference(paired_left, paired_right, unpaired_left, unpaired_right, out_weight, out_bias, chain_lengths, unpaired_depths):
    chain_of, depth_of = chain_tables(chain_lengths, unpaired_depths)
    free_ids = jnp.arange(DMAX, dtype=jnp.int32)
    live = (free_ids[:, None] < depth_of[None, :]).astype(unpaired_left.dtype)
    masked_left = unpaired_left * live[:, None, :]
    paired_group = S_P // N_SEQ
    free_group = DMAX // N_SEQ
    ref_rows = 8

    def one_block(block_index):
        offset = (block_index * ref_rows).astype(jnp.int32)
        chain_block = lax.dynamic_slice_in_dim(chain_of, offset, ref_rows, 0)
        depth_block = lax.dynamic_slice_in_dim(depth_of, offset, ref_rows, 0)
        same_chain = (chain_block[:, None] == chain_of[None, :]).astype(jnp.float32)
        summed = jnp.zeros((ref_rows, N, Z), jnp.float32)
        for group in range(N_SEQ):
            left_pair = lax.dynamic_slice_in_dim(paired_left[group * paired_group:(group + 1) * paired_group], offset, ref_rows, 2).astype(jnp.float32)
            right_pair = paired_right[group * paired_group:(group + 1) * paired_group].astype(jnp.float32)
            left_free = lax.dynamic_slice_in_dim(masked_left[group * free_group:(group + 1) * free_group], offset, ref_rows, 2).astype(jnp.float32)
            right_free = unpaired_right[group * free_group:(group + 1) * free_group].astype(jnp.float32)
            outer = jnp.einsum('sci,sdj->ijcd', left_pair, right_pair)
            outer = outer + jnp.einsum('sci,sdj->ijcd', left_free, right_free) * same_chain[:, :, None, None]
            outer_product = outer.astype(jnp.bfloat16).reshape(ref_rows * N, C * C)
            summed = summed + jnp.dot(outer_product, out_weight, preferred_element_type=jnp.float32).reshape(ref_rows, N, Z)
        denominator = S_P + same_chain * depth_block[:, None].astype(jnp.float32)
        return (summed / denominator[:, :, None] + out_bias).astype(jnp.bfloat16)

    blocks = lax.map(one_block, jnp.arange(N // ref_rows, dtype=jnp.int32))
    return blocks.reshape(N, N, Z)
```

```python
import functools

import jax
import jax.numpy as jnp
from jax import lax
from jax.experimental import pallas as pl
from jax.experimental.pallas import tpu as pltpu
from jax.sharding import PartitionSpec as P

S_P = 512
F32 = jnp.float32
BF16 = jnp.bfloat16
VM = pltpu.VMEM
SM = pltpu.SMEM


def vmem():
    return pl.BlockSpec(memory_space=VM)


def smem():
    return pl.BlockSpec(memory_space=SM)


def hbm():
    return pl.BlockSpec(memory_space=pl.ANY)


def limit(mib):
    return pltpu.CompilerParams(vmem_limit_bytes=mib * 1024 * 1024)


SCALARS = 6
PACK_STEP = 6


def chain_count(where_ref):
    return (where_ref.shape[0] - SCALARS) // 2


def chain_ends(where_ref):
    ends, total = [], jnp.int32(0)
    for k in range(chain_count(where_ref)):
        total = total + where_ref[SCALARS + k]
        ends.append(total)
    return ends


def chain_at(ends, position):
    found = (position >= ends[0]).astype(jnp.int32)
    for end in ends[1:]:
        found = found + (position >= end).astype(jnp.int32)
    return found


def depth_at(chain, where_ref):
    depth = jnp.zeros_like(chain)
    chains = chain_count(where_ref)
    for k in range(chains):
        depth = jnp.where(chain == k, where_ref[SCALARS + chains + k], depth)
    return depth


def fetch(sems, *pairs):
    copies = [pltpu.make_async_copy(src, dst, sems.at[k]) for k, (src, dst) in enumerate(pairs)]
    for one in copies:
        one.start()
    for one in copies:
        one.wait()


def right_kernel(where_ref, pair_hbm, free_hbm, own_ref, other_ref, pair_ref, free_ref, sems, pair_scr, free_scr):
    fetch(sems, (pair_hbm, pair_ref), (free_hbm, free_ref))
    sp, c, cols = pair_ref.shape
    sf = free_ref.shape[0]
    pair_scr[...] = pair_ref[...].astype(F32).reshape(sp * c, cols)
    free_scr[...] = free_ref[...].astype(F32).reshape(sf * c, cols)
    first = where_ref[0] == 0
    half = cols // 2
    for scr, rows, at in ((pair_scr, sp, 0), (free_scr, sf, sp)):
        lane = lax.broadcasted_iota(jnp.int32, (rows, cols), 1)
        low = lane < half
        for m in range(c // 2):
            lo = scr[pl.ds(m, rows, stride=c), :]
            hi = scr[pl.ds(m + c // 2, rows, stride=c), :]
            zero = jnp.where(low, lo, pltpu.roll(hi, half, 1)).astype(BF16)
            one = jnp.where(low, pltpu.roll(lo, half, 1), hi).astype(BF16)
            mp, t = m % (c // 4), m // (c // 4)
            lanes = slice(t * cols, (t + 1) * cols)
            own_ref[mp, at : at + rows, lanes] = jnp.where(first, zero, one)
            other_ref[mp, at : at + rows, lanes] = jnp.where(first, one, zero)


def left_kernel(
    where_ref, pair_hbm, free_hbm, weight_hbm, out_ref, turned_ref, pair_ref, free_ref, weight_ref, sems, *scratch
):
    pair_scr, free_scr, live_scr, weight_scr, sorted_scr = scratch
    fetch(sems, (weight_hbm, weight_ref), (pair_hbm, pair_ref), (free_hbm, free_ref))
    c, here, sp = pair_ref.shape
    weight_scr[...] = weight_ref[...].astype(F32)
    z = weight_ref.shape[1]
    for b in range(2):
        for m in range(c // 2):
            at = ((m % (c // 4)) * 2 + m // (c // 4)) * c
            sorted_scr[at : at + c, :] = weight_scr[pl.ds(m + b * c // 2, c, stride=c), :]
        turned_ref[b * z : (b + 1) * z, :] = sorted_scr[...].T.astype(BF16)
    sf = free_ref.shape[2]
    pair_scr[...] = pair_ref[...].astype(F32).reshape(c * here, sp)
    free_scr[...] = free_ref[...].astype(F32).reshape(c * here, sf)
    ends = chain_ends(where_ref)
    position = where_ref[1] + lax.broadcasted_iota(jnp.int32, (here, sf), 0)
    depth = depth_at(chain_at(ends, position), where_ref)
    row = where_ref[2] + lax.broadcasted_iota(jnp.int32, (here, sf), 1)
    live_scr[...] = (row < depth).astype(F32)
    for i in range(here // 2):
        a = pair_scr[pl.ds(i, c, stride=here), :]
        b = pair_scr[pl.ds(i + here // 2, c, stride=here), :]
        rows = jnp.concatenate([a, b], axis=1).astype(BF16)
        out_ref[i * c : (i + 1) * c, :] = rows
    base = here * c // 2
    for i in range(here):
        rows = (free_scr[pl.ds(i, c, stride=here), :] * live_scr[i : i + 1, :]).astype(BF16)
        out_ref[base + i * c : base + (i + 1) * c, :] = rows


def main_kernel(steps, *refs):
    where_ref, bias_ref, weight_ref, mine_ref, theirs_ref = refs[:5]
    shards = refs[5 : 5 + 4 * steps]
    rest = refs[5 + len(shards) :]
    out_ref, left_scr, pair_left, pair_scr, free_scr, x_scr, same_scr, inv_scr, sems = rest
    devices = 2 * steps
    here = out_ref.shape[0]
    cols = out_ref.shape[1]
    quarters = left_scr.shape[1]
    me = where_ref[3]
    sp = pair_scr.shape[1] // (2 * devices)
    sf = free_scr.shape[1] // (2 * devices)
    per = devices // quarters
    copies = []

    def copy(src, dst):
        one = pltpu.make_async_copy(src, dst, sems.at[len(copies)])
        one.start()
        copies.append(one)

    copy(mine_ref, left_scr.at[0])
    copy(theirs_ref, left_scr.at[1])

    def place(shard, which, offset):
        source = lax.rem(me + devices + offset, devices)
        quarter, at = source // per, lax.rem(source, per)
        block = (quarter * 2 + which) * per + at
        copy(shard.at[:, :sp, :], pair_scr.at[:, pl.ds(pl.multiple_of(block * sp, sp), sp), :])
        copy(shard.at[:, sp:, :], free_scr.at[:, pl.ds(pl.multiple_of(block * sf, sf), sf), :])

    blocks = pair_scr.shape[0]
    at = 0
    for which in range(2):
        place(shards[at], which, 0)
        at += 1
        for d in range(1, steps):
            place(shards[at], which, -d)
            place(shards[at + 1], which, d)
            at += 2
        place(shards[at], which, steps)
        at += 1

    ends = chain_ends(where_ref)
    first_row, first_col = where_ref[1], where_ref[4]
    wide = same_scr.shape[1]
    lane = lax.rem(lax.broadcasted_iota(jnp.int32, (here, wide), 1), cols)
    row_chain = chain_at(ends, first_row + lax.broadcasted_iota(jnp.int32, (here, wide), 0))
    col_chain = chain_at(ends, first_col + lane)
    same = (row_chain == col_chain).astype(F32)
    same_scr[...] = same
    depth = depth_at(row_chain, where_ref).astype(F32)
    inv_scr[...] = 1.0 / (S_P + same * depth)
    col_low, col_high = chain_at(ends, first_col), chain_at(ends, first_col + cols - 1)

    for one in copies:
        one.wait()

    c = left_scr.shape[2] // (here + here // 2)
    half_rows = here // 2 * c
    k64 = left_scr.shape[3] // 2
    for q in range(quarters):
        a = left_scr[0, q, :half_rows, :].astype(F32)
        b = left_scr[1, q, :half_rows, :].astype(F32)
        low = lax.broadcasted_iota(jnp.int32, a.shape, 1) < k64
        lanes = slice(q * 2 * k64, (q + 1) * 2 * k64)
        pair_left[:half_rows, lanes] = jnp.where(low, a, pltpu.roll(b, k64, 1)).astype(BF16)
        pair_left[half_rows:, lanes] = jnp.where(low, pltpu.roll(a, k64, 1), b).astype(BF16)

    tile = 8
    rows = tile * c
    z = out_ref.shape[2]
    weights = weight_ref[...]
    bias = bias_ref[...]

    def store_x(result, mp):
        for i in range(tile):
            for t in range(2):
                x_scr[i // 2, (mp * 2 + t) * c : (mp * 2 + t + 1) * c, (i % 2) * z : (i % 2 + 1) * z] = result[
                    i * c : (i + 1) * c, t * z : (t + 1) * z
                ].astype(BF16)

    def one_block(ib, carry):
        start = pl.multiple_of(ib * rows, rows)
        pair_lhs = pair_left[pl.ds(start, rows), :]
        row_low = chain_at(ends, first_row + ib * tile)
        row_high = chain_at(ends, first_row + ib * tile + tile - 1)
        meets = jnp.logical_and(row_low <= col_high, row_high >= col_low)

        @pl.when(meets)
        def _():
            free_lhs = jnp.concatenate(
                [left_scr[w, q, pl.ds(half_rows + start, rows), :] for q in range(quarters) for w in range(2)], axis=1
            )
            mask = same_scr[pl.ds(pl.multiple_of(ib * tile, tile), tile), :]
            mask = jnp.broadcast_to(mask[:, None, :], (tile, c, wide)).reshape(rows, wide)
            for mp in range(blocks):
                free = jnp.dot(free_lhs, free_scr[mp], preferred_element_type=F32)
                pair = jnp.dot(pair_lhs, pair_scr[mp], preferred_element_type=F32)
                store_x(pair + free * mask, mp)

        @pl.when(jnp.logical_not(meets))
        def _():
            for mp in range(blocks):
                store_x(jnp.dot(pair_lhs, pair_scr[mp], preferred_element_type=F32), mp)

        low = lax.broadcasted_iota(jnp.int32, (z, 2 * cols), 1) < cols
        inv = inv_scr[pl.ds(pl.multiple_of(ib * tile, tile), tile), : 2 * cols]
        for pair_of in range(tile // 2):
            d = jnp.dot(weights, x_scr[pair_of], preferred_element_type=F32)
            for i in range(2):
                lanes = slice(i * z, (i + 1) * z)
                picked = jnp.where(low, d[:z, lanes], d[z:, lanes])
                at = pair_of * 2 + i
                turned = (picked * inv[at : at + 1]).T
                out_ref[ib * tile + at] = (turned[:cols] + turned[cols:] + bias).astype(BF16)
        return carry

    lax.fori_loop(0, here // tile, one_block, 0)


def pack_kernel(where_ref, *refs):
    *parts, out_ref, sems = refs
    count = len(parts)
    me = where_ref[5]
    copies = []
    for k, part in enumerate(parts):
        copies.append(pltpu.make_async_copy(part, out_ref.at[lax.rem(me + count - k, count)], sems.at[k]))
        copies[-1].start()
    for one in copies:
        one.wait()


def body(
    paired_left,
    paired_right,
    unpaired_left,
    unpaired_right,
    out_weight,
    out_bias,
    chain_lengths,
    unpaired_depths,
):
    sp, c, cols = paired_right.shape
    sf = unpaired_right.shape[0]
    here = paired_left.shape[2]
    row_parts, col_parts = lax.axis_size("row"), lax.axis_size("col")
    seq, row, col = lax.axis_index("seq"), lax.axis_index("row"), lax.axis_index("col")
    half_cols = cols // 2
    z = out_weight.shape[1]
    left_sp, left_sf = paired_left.shape[0], unpaired_left.shape[0]
    where = jnp.stack(
        [
            seq,
            row * here,
            (seq * col_parts + col) * left_sf,
            row,
            col * cols + seq * half_cols,
            col,
        ]
    ).astype(jnp.int32)
    where = jnp.concatenate([where, chain_lengths, unpaired_depths])

    shard_shape = jax.ShapeDtypeStruct((c // 4, sp + sf, 2 * cols), BF16)
    own, other = pl.pallas_call(
        right_kernel,
        out_shape=(shard_shape, shard_shape),
        in_specs=[smem(), hbm(), hbm()],
        out_specs=(vmem(), vmem()),
        scratch_shapes=[
            VM(paired_right.shape, BF16),
            VM(unpaired_right.shape, BF16),
            pltpu.SemaphoreType.DMA((2,)),
            VM((sp * c, cols), F32),
            VM((sf * c, cols), F32),
        ],
        compiler_params=limit(6),
    )(where, paired_right, unpaired_right)
    swap = [(0, 1), (1, 0)]
    partner = lax.ppermute(other, "seq", swap)
    up = [(i, (i + 1) % row_parts) for i in range(row_parts)]
    down = [(i, (i - 1) % row_parts) for i in range(row_parts)]
    steps = row_parts // 2
    tied = lax.optimization_barrier
    send = lambda pair: (lax.ppermute(pair[0], "row", up), lax.ppermute(pair[1], "row", down))
    shift = lambda x, k: lax.ppermute(x, "col", [(i, (i + k) % col_parts) for i in range(col_parts)])

    def after(values, *earlier):
        return tied((*values, *earlier))[: len(values)]

    own_ring, par_ring = [own], [partner]
    own_at = send((own, own))
    par_at = send((partner, partner))
    own_ring += own_at
    par_ring += par_at
    paired_left, unpaired_left, out_weight = after((paired_left, unpaired_left, out_weight), own_at[0])
    left, weight = pl.pallas_call(
        left_kernel,
        out_shape=(
            jax.ShapeDtypeStruct((here * c * 3 // 2, left_sf), BF16),
            jax.ShapeDtypeStruct((2 * z, c * c // 2), BF16),
        ),
        in_specs=[smem(), hbm(), hbm(), hbm()],
        out_specs=(vmem(), vmem()),
        scratch_shapes=[
            VM((c, here, left_sp), BF16),
            VM((c, here, left_sf), BF16),
            VM(out_weight.shape, BF16),
            pltpu.SemaphoreType.DMA((3,)),
            VM((c * here, left_sp), F32),
            VM((c * here, left_sf), F32),
            VM((here, left_sf), F32),
            VM((c * c, z), F32),
            VM((c * c // 2, z), F32),
        ],
        compiler_params=limit(10),
    )(
        where,
        jnp.transpose(paired_left, (1, 2, 0)),
        jnp.transpose(unpaired_left, (1, 2, 0)),
        out_weight,
    )
    left_parts = [left]
    for k in range(2, steps + 1):
        before = [par_ring[-3] if k > 2 else partner]
        if k == 3:
            before.append(left)
        if 3 < k <= 3 + col_parts - 1:
            before.append(left_parts[k - 3])
        if k == PACK_STEP + 2:
            before.append(mine)
        own_at = after(own_at, *before)
        par_at = after(par_at, own_ring[-1])
        if k < steps:
            own_at, par_at = send(own_at), send(par_at)
        else:
            own_at, par_at = send(own_at)[:1], send(par_at)[1:]
        own_ring += own_at
        par_ring += par_at
        if k < 2 + col_parts - 1:
            left_parts.append(shift(after((left,), par_ring[2 * k - 3])[0], k - 1))
        if k == PACK_STEP:
            mine = pl.pallas_call(
                pack_kernel,
                out_shape=jax.ShapeDtypeStruct((col_parts, *left.shape), BF16),
                in_specs=[smem()] + [vmem()] * col_parts,
                out_specs=vmem(),
                scratch_shapes=[pltpu.SemaphoreType.DMA((col_parts,))],
                compiler_params=limit(2),
            )(where, *after(left_parts, own_ring[-3]))
            theirs = lax.ppermute(mine, "seq", swap)
    rings = own_ring + par_ring

    seqs = 2
    n_copies = 2 + 2 * len(rings)
    return pl.pallas_call(
        functools.partial(main_kernel, steps),
        out_shape=jax.ShapeDtypeStruct((here, half_cols, z), BF16),
        in_specs=[smem(), vmem(), vmem(), vmem(), vmem()] + [vmem()] * len(rings),
        out_specs=vmem(),
        scratch_shapes=[
            VM((seqs, *mine.shape), BF16),
            VM((here * c, seqs * col_parts * left_sp), BF16),
            VM((c // 4, seqs * row_parts * sp, 2 * cols), BF16),
            VM((c // 4, seqs * row_parts * sf, 2 * cols), BF16),
            VM((4, c * c // 2, 2 * z), BF16),
            VM((here, 2 * cols), F32),
            VM((here, 2 * cols), F32),
            pltpu.SemaphoreType.DMA((n_copies,)),
        ],
        compiler_params=limit(18),
    )(where, out_bias.reshape(1, z), weight, mine, theirs, *rings)


def solution(mesh):
    return jax.shard_map(
        body,
        mesh=mesh,
        in_specs=(
            P(("groups", "seq", "col"), None, "row"),
            P(("groups", "seq", "row"), None, "col"),
            P(("groups", "seq", "col"), None, "row"),
            P(("groups", "seq", "row"), None, "col"),
            P(),
            P(),
            P("groups"),
            P("groups"),
        ),
        out_specs=P(("groups", "row"), ("col", "seq"), None),
        check_vma=False,
    )
```

```python
import functools

import jax
import jax.numpy as jnp
from jax import lax
from jax.experimental import pallas as pl
from jax.experimental.pallas import tpu as pltpu
from jax.sharding import PartitionSpec as P

S_P = 512
F32 = jnp.float32
BF16 = jnp.bfloat16
VM = pltpu.VMEM
SM = pltpu.SMEM


def vmem():
    return pl.BlockSpec(memory_space=VM)


def smem():
    return pl.BlockSpec(memory_space=SM)


def hbm():
    return pl.BlockSpec(memory_space=pl.ANY)


def limit(mib):
    return pltpu.CompilerParams(vmem_limit_bytes=mib * 1024 * 1024)


SCALARS = 7
PACK_STEP = 6


def chain_count(where_ref):
    return (where_ref.shape[0] - SCALARS) // 2


def chain_ends(where_ref):
    ends, total = [], jnp.int32(0)
    for k in range(chain_count(where_ref)):
        total = total + where_ref[SCALARS + k]
        ends.append(total)
    return ends


def chain_at(ends, position):
    found = (position >= ends[0]).astype(jnp.int32)
    for end in ends[1:]:
        found = found + (position >= end).astype(jnp.int32)
    return found


def depth_at(chain, where_ref):
    depth = jnp.zeros_like(chain)
    chains = chain_count(where_ref)
    for k in range(chains):
        depth = jnp.where(chain == k, where_ref[SCALARS + chains + k], depth)
    return depth


def fetch(sems, *pairs):
    copies = [pltpu.make_async_copy(src, dst, sems.at[k]) for k, (src, dst) in enumerate(pairs)]
    for one in copies:
        one.start()
    for one in copies:
        one.wait()


def right_kernel(where_ref, pair_hbm, free_hbm, own_ref, other_ref, pair_ref, free_ref, sems, pair_scr, free_scr):
    fetch(sems, (pair_hbm, pair_ref), (free_hbm, free_ref))
    sp, c, cols = pair_ref.shape
    sf = free_ref.shape[0]
    pair_scr[...] = pair_ref[...].astype(F32).reshape(sp * c, cols)
    free_scr[...] = free_ref[...].astype(F32).reshape(sf * c, cols)
    first = where_ref[0] == 0
    half = cols // 2
    for scr, rows, at in ((pair_scr, sp, 0), (free_scr, sf, sp)):
        lane = lax.broadcasted_iota(jnp.int32, (rows, cols), 1)
        low = lane < half
        for m in range(c // 2):
            lo = scr[pl.ds(m, rows, stride=c), :]
            hi = scr[pl.ds(m + c // 2, rows, stride=c), :]
            zero = jnp.where(low, lo, pltpu.roll(hi, half, 1)).astype(BF16)
            one = jnp.where(low, pltpu.roll(lo, half, 1), hi).astype(BF16)
            mp, t = m % (c // 4), m // (c // 4)
            lanes = slice(t * cols, (t + 1) * cols)
            own_ref[mp, at : at + rows, lanes] = jnp.where(first, zero, one)
            other_ref[mp, at : at + rows, lanes] = jnp.where(first, one, zero)


def left_kernel(
    where_ref, pair_hbm, free_hbm, weight_hbm, out_ref, turned_ref, pair_ref, free_ref, weight_ref, sems, *scratch
):
    pair_scr, free_scr, live_scr, weight_scr, sorted_scr = scratch
    fetch(sems, (weight_hbm, weight_ref), (pair_hbm, pair_ref), (free_hbm, free_ref))
    c, here, sp = pair_ref.shape
    weight_scr[...] = weight_ref[...].astype(F32)
    z = weight_ref.shape[1]
    for b in range(2):
        for m in range(c // 2):
            at = ((m % (c // 4)) * 2 + m // (c // 4)) * c
            sorted_scr[at : at + c, :] = weight_scr[pl.ds(m + b * c // 2, c, stride=c), :]
        turned_ref[b * z : (b + 1) * z, :] = sorted_scr[...].T.astype(BF16)
    sf = free_ref.shape[2]
    pair_scr[...] = pair_ref[...].astype(F32).reshape(c * here, sp)
    free_scr[...] = free_ref[...].astype(F32).reshape(c * here, sf)
    ends = chain_ends(where_ref)
    position = where_ref[1] + lax.broadcasted_iota(jnp.int32, (here, sf), 0)
    depth = depth_at(chain_at(ends, position), where_ref)
    row = where_ref[2] + lax.broadcasted_iota(jnp.int32, (here, sf), 1)
    live_scr[...] = (row < depth).astype(F32)
    for i in range(here // 2):
        a = pair_scr[pl.ds(i, c, stride=here), :]
        b = pair_scr[pl.ds(i + here // 2, c, stride=here), :]
        rows = jnp.concatenate([a, b], axis=1).astype(BF16)
        out_ref[i * c : (i + 1) * c, :] = rows
    base = here * c // 2
    for i in range(here):
        rows = (free_scr[pl.ds(i, c, stride=here), :] * live_scr[i : i + 1, :]).astype(BF16)
        out_ref[base + i * c : base + (i + 1) * c, :] = rows


def quarter_at(quarter, mine):
    step = lax.rem(quarter - mine + 4, 4)
    return jnp.where(step == 2, 3, jnp.where(step == 3, 2, step))


def same_chain(where_ref, shape, cols):
    ends = chain_ends(where_ref)
    lane = lax.rem(lax.broadcasted_iota(jnp.int32, shape, 1), cols)
    row_chain = chain_at(ends, where_ref[1] + lax.broadcasted_iota(jnp.int32, shape, 0))
    same = (row_chain == chain_at(ends, where_ref[4] + lane)).astype(F32)
    return same, row_chain


def block_meets(where_ref, ib, tile, cols):
    ends = chain_ends(where_ref)
    first_row = where_ref[1] + ib * tile
    first_col = where_ref[4]
    return jnp.logical_and(
        chain_at(ends, first_row) <= chain_at(ends, first_col + cols - 1),
        chain_at(ends, first_row + tile - 1) >= chain_at(ends, first_col),
    )


def block_mask(same_scr, ib, tile, c):
    mask = same_scr[pl.ds(pl.multiple_of(ib * tile, tile), tile), :]
    wide = mask.shape[1]
    return jnp.broadcast_to(mask[:, None, :], (tile, c, wide)).reshape(tile * c, wide)


def early_kernel(steps, cols, *refs):
    where_ref, mine_ref, theirs_ref = refs[:3]
    shards = refs[3 : 3 + 2 * (2 * steps - 1)]
    sum_ref, far_left, far_pair, far_free, near_left, near_pair, near_free, same_scr, sems = refs[3 + len(shards) :]
    devices = 2 * steps
    quarters = mine_ref.shape[0]
    per = devices // quarters
    here = same_scr.shape[0]
    c = mine_ref.shape[1] // (here + here // 2)
    me = where_ref[3]
    my_quarter = me // per
    near = quarters - 1

    def place(shard, which, offset, slot):
        source = lax.rem(me + devices + offset, devices)
        to = quarter_at(source // per, my_quarter)
        at = lax.rem(source, per)

        @pl.when(to < near)
        def _():
            near_at = jnp.minimum(to, near - 1)
            start(shard, near_pair.at[near_at], near_free.at[near_at], which, at, slot)

        @pl.when(to == near)
        def _():
            start(shard, far_pair, far_free, which, at, slot)

    def start(shard, pair_dst, free_dst, which, at, slot):
        for one in pieces(shard, pair_dst, free_dst, which, at, slot):
            one.start()

    def pieces(shard, pair_dst, free_dst, which, at, slot):
        sp = pair_dst.shape[1] // (2 * per)
        sf = free_dst.shape[1] // (2 * per)
        block = which * per + at
        return (
            pltpu.make_async_copy(
                shard.at[:, :sp, :], pair_dst.at[:, pl.ds(pl.multiple_of(block * sp, sp), sp), :], sems.at[2 * slot]
            ),
            pltpu.make_async_copy(
                shard.at[:, sp:, :], free_dst.at[:, pl.ds(pl.multiple_of(block * sf, sf), sf), :], sems.at[2 * slot + 1]
            ),
        )

    offsets = [0] + [sign * d for d in range(1, steps) for sign in (-1, 1)]
    for which in range(2):
        for k, offset in enumerate(offsets):
            place(shards[which * len(offsets) + k], which, offset, which * len(offsets) + k)

    same, _ = same_chain(where_ref, same_scr.shape, cols)
    same_scr[...] = same
    half_rows = here // 2 * c
    k64 = mine_ref.shape[2] // 2
    for q in range(quarters):
        a = mine_ref[q, :half_rows, :].astype(F32)
        b = theirs_ref[q, :half_rows, :].astype(F32)
        low = lax.broadcasted_iota(jnp.int32, a.shape, 1) < k64
        top = jnp.where(low, a, pltpu.roll(b, k64, 1)).astype(BF16)
        bottom = jnp.where(low, pltpu.roll(a, k64, 1), b).astype(BF16)
        if q < near:
            near_left[:half_rows, q * 2 * k64 : (q + 1) * 2 * k64] = top
            near_left[half_rows:, q * 2 * k64 : (q + 1) * 2 * k64] = bottom
        else:
            far_left[:half_rows, :] = top
            far_left[half_rows:, :] = bottom

    for slot, shard in enumerate(shards):
        for one in pieces(shard, near_pair.at[0], near_free.at[0], 0, 0, slot):
            one.wait()

    tile = 8
    rows = tile * c
    blocks = near_pair.shape[1]

    def one_block(ib, carry):
        at = pl.multiple_of(ib * rows, rows)
        pair_lhs = near_left[pl.ds(at, rows), :]
        meets = block_meets(where_ref, ib, tile, cols)

        def pair_dot(mp):
            rhs = jnp.concatenate([near_pair[q, mp] for q in range(near)], axis=0)
            return jnp.dot(pair_lhs, rhs, preferred_element_type=F32)

        @pl.when(meets)
        def _():
            lhs = jnp.concatenate(
                [ref[q, pl.ds(half_rows + at, rows), :] for q in range(near) for ref in (mine_ref, theirs_ref)], axis=1
            )
            mask = block_mask(same_scr, ib, tile, c)
            for mp in range(blocks):
                rhs = jnp.concatenate([near_free[q, mp] for q in range(near)], axis=0)
                free = jnp.dot(lhs, rhs, preferred_element_type=F32)
                sum_ref[mp, pl.ds(at, rows), :] = pair_dot(mp) + free * mask

        @pl.when(jnp.logical_not(meets))
        def _():
            for mp in range(blocks):
                sum_ref[mp, pl.ds(at, rows), :] = pair_dot(mp)

        return carry

    lax.fori_loop(0, here // tile, one_block, 0)


def late_kernel(*refs):
    (where_ref, bias_ref, weight_ref, mine_ref, theirs_ref, sum_ref, far_left, _, _, own_ref, par_ref) = refs[:11]
    out_ref, far_pair, far_free, x_scr, same_scr, inv_scr, sems = refs[11:]
    here, cols, z = out_ref.shape
    quarters = mine_ref.shape[0]
    c = mine_ref.shape[1] // (here + here // 2)
    half_rows = here // 2 * c
    sp = far_pair.shape[1] // (2 * quarters)
    sf = far_free.shape[1] // (2 * quarters)
    at = lax.rem(where_ref[3], quarters)
    copies = []
    for which, shard in enumerate((own_ref, par_ref)):
        block = which * quarters + at
        for src, dst in (
            (shard.at[:, :sp, :], far_pair.at[:, pl.ds(pl.multiple_of(block * sp, sp), sp), :]),
            (shard.at[:, sp:, :], far_free.at[:, pl.ds(pl.multiple_of(block * sf, sf), sf), :]),
        ):
            copies.append(pltpu.make_async_copy(src, dst, sems.at[len(copies)]))
            copies[-1].start()
    same, row_chain = same_chain(where_ref, same_scr.shape, cols)
    same_scr[...] = same
    inv_scr[...] = 1.0 / (S_P + same * depth_at(row_chain, where_ref).astype(F32))
    weights = weight_ref[...]
    bias = bias_ref[...]
    for one in copies:
        one.wait()

    tile = 8
    rows = tile * c
    blocks = far_pair.shape[0]
    width = 2 * cols
    last = quarters - 1

    def store_x(result, mp):
        for i in range(tile):
            for t in range(2):
                x_scr[
                    i // 2, (mp * 2 + t) * c : (mp * 2 + t + 1) * c, (i % 2) * width : (i % 2 + 1) * width
                ] = result[i * c : (i + 1) * c, t * width : (t + 1) * width].astype(BF16)

    def one_block(ib, carry):
        at = pl.multiple_of(ib * rows, rows)
        pair_lhs = far_left[pl.ds(at, rows), :]
        meets = block_meets(where_ref, ib, tile, cols)

        def pair_sum(mp):
            return sum_ref[mp, pl.ds(at, rows), :] + jnp.dot(pair_lhs, far_pair[mp], preferred_element_type=F32)

        @pl.when(meets)
        def _():
            lhs = jnp.concatenate([ref[last, pl.ds(half_rows + at, rows), :] for ref in (mine_ref, theirs_ref)], axis=1)
            mask = block_mask(same_scr, ib, tile, c)
            for mp in range(blocks):
                free = jnp.dot(lhs, far_free[mp], preferred_element_type=F32)
                store_x(pair_sum(mp) + free * mask, mp)

        @pl.when(jnp.logical_not(meets))
        def _():
            for mp in range(blocks):
                store_x(pair_sum(mp), mp)

        low = lax.broadcasted_iota(jnp.int32, (z, width), 1) < cols
        inv = inv_scr[pl.ds(pl.multiple_of(ib * tile, tile), tile), :width]
        for pair_of in range(tile // 2):
            d = jnp.dot(weights, x_scr[pair_of], preferred_element_type=F32)
            for i in range(2):
                lanes = slice(i * width, (i + 1) * width)
                picked = jnp.where(low, d[:z, lanes], d[z:, lanes])
                row = pair_of * 2 + i
                turned = (picked * inv[row : row + 1]).T
                out_ref[ib * tile + row] = (turned[:cols] + turned[cols:] + bias).astype(BF16)
        return carry

    lax.fori_loop(0, here // tile, one_block, 0)


def pack_kernel(where_ref, *refs):
    *parts, out_ref, sems = refs
    count = len(parts)
    me, my_quarter = where_ref[5], where_ref[6]
    copies = []
    for k, part in enumerate(parts):
        to = quarter_at(lax.rem(me + count - k, count), my_quarter)
        copies.append(pltpu.make_async_copy(part, out_ref.at[to], sems.at[k]))
        copies[-1].start()
    for one in copies:
        one.wait()


def body(
    paired_left,
    paired_right,
    unpaired_left,
    unpaired_right,
    out_weight,
    out_bias,
    chain_lengths,
    unpaired_depths,
):
    sp, c, cols = paired_right.shape
    sf = unpaired_right.shape[0]
    here = paired_left.shape[2]
    row_parts, col_parts = lax.axis_size("row"), lax.axis_size("col")
    seq, row, col = lax.axis_index("seq"), lax.axis_index("row"), lax.axis_index("col")
    half_cols = cols // 2
    z = out_weight.shape[1]
    left_sp, left_sf = paired_left.shape[0], unpaired_left.shape[0]
    where = jnp.stack(
        [
            seq,
            row * here,
            (seq * col_parts + col) * left_sf,
            row,
            col * cols + seq * half_cols,
            col,
            row // (row_parts // col_parts),
        ]
    ).astype(jnp.int32)
    where = jnp.concatenate([where, chain_lengths, unpaired_depths])

    shard_shape = jax.ShapeDtypeStruct((c // 4, sp + sf, 2 * cols), BF16)
    own, other = pl.pallas_call(
        right_kernel,
        out_shape=(shard_shape, shard_shape),
        in_specs=[smem(), hbm(), hbm()],
        out_specs=(vmem(), vmem()),
        scratch_shapes=[
            VM(paired_right.shape, BF16),
            VM(unpaired_right.shape, BF16),
            pltpu.SemaphoreType.DMA((2,)),
            VM((sp * c, cols), F32),
            VM((sf * c, cols), F32),
        ],
        compiler_params=limit(6),
    )(where, paired_right, unpaired_right)
    swap = [(0, 1), (1, 0)]
    partner = lax.ppermute(other, "seq", swap)
    up = [(i, (i + 1) % row_parts) for i in range(row_parts)]
    down = [(i, (i - 1) % row_parts) for i in range(row_parts)]
    steps = row_parts // 2
    tied = lax.optimization_barrier
    send = lambda pair: (lax.ppermute(pair[0], "row", up), lax.ppermute(pair[1], "row", down))
    shift = lambda x, k: lax.ppermute(x, "col", [(i, (i + k) % col_parts) for i in range(col_parts)])

    def after(values, *earlier):
        return tied((*values, *earlier))[: len(values)]

    own_ring, par_ring = [own], [partner]
    own_at = send((own, own))
    par_at = send((partner, partner))
    own_ring += own_at
    par_ring += par_at
    paired_left, unpaired_left, out_weight = after((paired_left, unpaired_left, out_weight), own_at[0])
    left, weight = pl.pallas_call(
        left_kernel,
        out_shape=(
            jax.ShapeDtypeStruct((here * c * 3 // 2, left_sf), BF16),
            jax.ShapeDtypeStruct((2 * z, c * c // 2), BF16),
        ),
        in_specs=[smem(), hbm(), hbm(), hbm()],
        out_specs=(vmem(), vmem()),
        scratch_shapes=[
            VM((c, here, left_sp), BF16),
            VM((c, here, left_sf), BF16),
            VM(out_weight.shape, BF16),
            pltpu.SemaphoreType.DMA((3,)),
            VM((c * here, left_sp), F32),
            VM((c * here, left_sf), F32),
            VM((here, left_sf), F32),
            VM((c * c, z), F32),
            VM((c * c // 2, z), F32),
        ],
        compiler_params=limit(10),
    )(
        where,
        jnp.transpose(paired_left, (1, 2, 0)),
        jnp.transpose(unpaired_left, (1, 2, 0)),
        out_weight,
    )
    left_parts = [left]
    for k in range(2, steps + 1):
        before = [par_ring[-3] if k > 2 else partner]
        if k == 3:
            before.append(left)
        if 3 < k <= 3 + col_parts - 1:
            before.append(left_parts[k - 3])
        if k == PACK_STEP + 2:
            before.append(mine)
        own_at = after(own_at, *before)
        par_at = after(par_at, own_ring[-1])
        if k < steps:
            own_at, par_at = send(own_at), send(par_at)
        else:
            own_at, par_at = send(own_at)[:1], send(par_at)[1:]
        own_ring += own_at
        par_ring += par_at
        if k < 2 + col_parts - 1:
            left_parts.append(shift(after((left,), par_ring[2 * k - 3])[0], k - 1))
        if k == PACK_STEP:
            mine = pl.pallas_call(
                pack_kernel,
                out_shape=jax.ShapeDtypeStruct((col_parts, *left.shape), BF16),
                in_specs=[smem()] + [vmem()] * col_parts,
                out_specs=vmem(),
                scratch_shapes=[pltpu.SemaphoreType.DMA((col_parts,))],
                compiler_params=limit(2),
            )(where, *after(left_parts, own_ring[-3]))
            theirs = lax.ppermute(mine, "seq", swap)
    rings = own_ring[:-1] + par_ring[:-1]
    wide = 2 * cols
    pair_rows, free_rows = 2 * left_sp, 2 * left_sf
    blocks = c // 4
    near = col_parts - 1
    total, far_left, far_pair, far_free = pl.pallas_call(
        functools.partial(early_kernel, steps, half_cols),
        out_shape=(
            jax.ShapeDtypeStruct((blocks, here * c, wide), F32),
            jax.ShapeDtypeStruct((here * c, pair_rows), BF16),
            jax.ShapeDtypeStruct((blocks, pair_rows, wide), BF16),
            jax.ShapeDtypeStruct((blocks, free_rows, wide), BF16),
        ),
        in_specs=[smem()] + [vmem()] * (2 + len(rings)),
        out_specs=(vmem(),) * 4,
        scratch_shapes=[
            VM((here * c, near * pair_rows), BF16),
            VM((near, blocks, pair_rows, wide), BF16),
            VM((near, blocks, free_rows, wide), BF16),
            VM((here, wide), F32),
            pltpu.SemaphoreType.DMA((2 * len(rings),)),
        ],
        compiler_params=limit(20),
    )(where, mine, theirs, *rings)
    result, _, _ = pl.pallas_call(
        late_kernel,
        out_shape=(
            jax.ShapeDtypeStruct((here, half_cols, z), BF16),
            jax.ShapeDtypeStruct(far_pair.shape, BF16),
            jax.ShapeDtypeStruct(far_free.shape, BF16),
        ),
        in_specs=[smem()] + [vmem()] * 10,
        out_specs=(vmem(),) * 3,
        input_output_aliases={7: 1, 8: 2},
        scratch_shapes=[
            VM((4, c * c // 2, wide), BF16),
            VM((here, wide), F32),
            VM((here, wide), F32),
            pltpu.SemaphoreType.DMA((4,)),
        ],
        compiler_params=limit(16),
    )(where, out_bias.reshape(1, z), weight, mine, theirs, total, far_left, far_pair, far_free, own_ring[-1], par_ring[-1])
    return result


def solution(mesh):
    return jax.shard_map(
        body,
        mesh=mesh,
        in_specs=(
            P(("groups", "seq", "col"), None, "row"),
            P(("groups", "seq", "row"), None, "col"),
            P(("groups", "seq", "col"), None, "row"),
            P(("groups", "seq", "row"), None, "col"),
            P(),
            P(),
            P("groups"),
            P("groups"),
        ),
        out_specs=P(("groups", "row"), ("col", "seq"), None),
        check_vma=False,
    )
```

```python
import functools

import jax
import jax.numpy as jnp
from jax import lax
from jax.experimental import pallas as pl
from jax.experimental.pallas import tpu as pltpu
from jax.sharding import PartitionSpec as P

S_P = 512
F32 = jnp.float32
BF16 = jnp.bfloat16
VM = pltpu.VMEM
SM = pltpu.SMEM


def vmem():
    return pl.BlockSpec(memory_space=VM)


def smem():
    return pl.BlockSpec(memory_space=SM)


def hbm():
    return pl.BlockSpec(memory_space=pl.ANY)


def limit(mib):
    return pltpu.CompilerParams(vmem_limit_bytes=mib * 1024 * 1024)


SCALARS = 7
PACK_STEP = 6
TOGETHER = 2


def chain_count(where_ref):
    return (where_ref.shape[0] - SCALARS) // 2


def chain_ends(where_ref):
    ends, total = [], jnp.int32(0)
    for k in range(chain_count(where_ref)):
        total = total + where_ref[SCALARS + k]
        ends.append(total)
    return ends


def chain_at(ends, position):
    found = (position >= ends[0]).astype(jnp.int32)
    for end in ends[1:]:
        found = found + (position >= end).astype(jnp.int32)
    return found


def depth_at(chain, where_ref):
    depth = jnp.zeros_like(chain)
    chains = chain_count(where_ref)
    for k in range(chains):
        depth = jnp.where(chain == k, where_ref[SCALARS + chains + k], depth)
    return depth


def fetch(sems, *pairs):
    copies = [pltpu.make_async_copy(src, dst, sems.at[k]) for k, (src, dst) in enumerate(pairs)]
    for one in copies:
        one.start()
    for one in copies:
        one.wait()


def right_kernel(where_ref, pair_hbm, free_hbm, own_ref, other_ref, pair_ref, free_ref, sems, pair_scr, free_scr):
    fetch(sems, (pair_hbm, pair_ref), (free_hbm, free_ref))
    sp, c, cols = pair_ref.shape
    sf = free_ref.shape[0]
    pair_scr[...] = pair_ref[...].astype(F32).reshape(sp * c, cols)
    free_scr[...] = free_ref[...].astype(F32).reshape(sf * c, cols)
    first = where_ref[0] == 0
    half = cols // 2
    for scr, rows, at in ((pair_scr, sp, 0), (free_scr, sf, sp)):
        lane = lax.broadcasted_iota(jnp.int32, (rows, cols), 1)
        low = lane < half
        for m in range(c // 2):
            lo = scr[pl.ds(m, rows, stride=c), :]
            hi = scr[pl.ds(m + c // 2, rows, stride=c), :]
            zero = jnp.where(low, lo, pltpu.roll(hi, half, 1)).astype(BF16)
            one = jnp.where(low, pltpu.roll(lo, half, 1), hi).astype(BF16)
            mp, t = m % (c // 4), m // (c // 4)
            lanes = slice(t * cols, (t + 1) * cols)
            own_ref[mp, at : at + rows, lanes] = jnp.where(first, zero, one)
            other_ref[mp, at : at + rows, lanes] = jnp.where(first, one, zero)


def left_kernel(
    where_ref, pair_hbm, free_hbm, weight_hbm, out_ref, turned_ref, pair_ref, free_ref, weight_ref, sems, *scratch
):
    pair_scr, free_scr, live_scr, weight_scr, sorted_scr = scratch
    fetch(sems, (weight_hbm, weight_ref), (pair_hbm, pair_ref), (free_hbm, free_ref))
    c, here, sp = pair_ref.shape
    weight_scr[...] = weight_ref[...].astype(F32)
    z = weight_ref.shape[1]
    for b in range(2):
        for m in range(c // 2):
            at = ((m % (c // 4)) * 2 + m // (c // 4)) * c
            sorted_scr[at : at + c, :] = weight_scr[pl.ds(m + b * c // 2, c, stride=c), :]
        turned_ref[b * z : (b + 1) * z, :] = sorted_scr[...].T.astype(BF16)
    sf = free_ref.shape[2]
    pair_scr[...] = pair_ref[...].astype(F32).reshape(c * here, sp)
    free_scr[...] = free_ref[...].astype(F32).reshape(c * here, sf)
    ends = chain_ends(where_ref)
    position = where_ref[1] + lax.broadcasted_iota(jnp.int32, (here, sf), 0)
    depth = depth_at(chain_at(ends, position), where_ref)
    row = where_ref[2] + lax.broadcasted_iota(jnp.int32, (here, sf), 1)
    live_scr[...] = (row < depth).astype(F32)
    for i in range(here // 2):
        a = pair_scr[pl.ds(i, c, stride=here), :]
        b = pair_scr[pl.ds(i + here // 2, c, stride=here), :]
        rows = jnp.concatenate([a, b], axis=1).astype(BF16)
        out_ref[i * c : (i + 1) * c, :] = rows
    base = here * c // 2
    for i in range(here):
        rows = (free_scr[pl.ds(i, c, stride=here), :] * live_scr[i : i + 1, :]).astype(BF16)
        out_ref[base + i * c : base + (i + 1) * c, :] = rows


def quarter_at(quarter, mine):
    step = lax.rem(quarter - mine + 4, 4)
    return jnp.where(step == 2, 3, jnp.where(step == 3, 2, step))


def same_chain(where_ref, shape, cols):
    ends = chain_ends(where_ref)
    lane = lax.rem(lax.broadcasted_iota(jnp.int32, shape, 1), cols)
    row_chain = chain_at(ends, where_ref[1] + lax.broadcasted_iota(jnp.int32, shape, 0))
    same = (row_chain == chain_at(ends, where_ref[4] + lane)).astype(F32)
    return same, row_chain


def block_meets(where_ref, ib, tile, cols):
    ends = chain_ends(where_ref)
    first_row = where_ref[1] + ib * tile
    first_col = where_ref[4]
    return jnp.logical_and(
        chain_at(ends, first_row) <= chain_at(ends, first_col + cols - 1),
        chain_at(ends, first_row + tile - 1) >= chain_at(ends, first_col),
    )


def block_mask(same_scr, ib, tile, c):
    mask = same_scr[pl.ds(pl.multiple_of(ib * tile, tile), tile), :]
    wide = mask.shape[1]
    return jnp.broadcast_to(mask[:, None, :], (tile, c, wide)).reshape(tile * c, wide)


def early_kernel(steps, cols, *refs):
    where_ref, mine_ref, theirs_ref = refs[:3]
    shards = refs[3 : 3 + 2 * (2 * steps - 1)]
    sum_ref, far_left, far_pair, far_free, near_left, near_pair, near_free, same_scr, sems = refs[3 + len(shards) :]
    devices = 2 * steps
    quarters = mine_ref.shape[0]
    per = devices // quarters
    here = same_scr.shape[0]
    c = mine_ref.shape[1] // (here + here // 2)
    me = where_ref[3]
    my_quarter = me // per
    near = quarters - 1

    def place(shard, which, offset, slot):
        source = lax.rem(me + devices + offset, devices)
        to = quarter_at(source // per, my_quarter)
        at = lax.rem(source, per)

        near_at = jnp.minimum(to, near - 1)
        if abs(offset) <= steps - per:
            start(shard, near_pair.at[near_at], near_free.at[near_at], which, at, slot)
            return

        @pl.when(to < near)
        def _():
            start(shard, near_pair.at[near_at], near_free.at[near_at], which, at, slot)

        @pl.when(to == near)
        def _():
            start(shard, far_pair, far_free, which, at, slot)

    def start(shard, pair_dst, free_dst, which, at, slot):
        for one in pieces(shard, pair_dst, free_dst, which, at, slot):
            one.start()

    def pieces(shard, pair_dst, free_dst, which, at, slot):
        sp = pair_dst.shape[1] // (2 * per)
        sf = free_dst.shape[1] // (2 * per)
        block = which * per + at
        return (
            pltpu.make_async_copy(
                shard.at[:, :sp, :], pair_dst.at[:, pl.ds(pl.multiple_of(block * sp, sp), sp), :], sems.at[2 * slot]
            ),
            pltpu.make_async_copy(
                shard.at[:, sp:, :], free_dst.at[:, pl.ds(pl.multiple_of(block * sf, sf), sf), :], sems.at[2 * slot + 1]
            ),
        )

    offsets = [0] + [sign * d for d in range(1, steps) for sign in (-1, 1)]
    for which in range(2):
        for k, offset in enumerate(offsets):
            place(shards[which * len(offsets) + k], which, offset, which * len(offsets) + k)

    same, _ = same_chain(where_ref, same_scr.shape, cols)
    same_scr[...] = same
    half_rows = here // 2 * c
    k64 = mine_ref.shape[2] // 2
    for q in range(quarters):
        a = mine_ref[q, :half_rows, :].astype(F32)
        b = theirs_ref[q, :half_rows, :].astype(F32)
        low = lax.broadcasted_iota(jnp.int32, a.shape, 1) < k64
        top = jnp.where(low, a, pltpu.roll(b, k64, 1)).astype(BF16)
        bottom = jnp.where(low, pltpu.roll(a, k64, 1), b).astype(BF16)
        if q < near:
            near_left[:half_rows, q * 2 * k64 : (q + 1) * 2 * k64] = top
            near_left[half_rows:, q * 2 * k64 : (q + 1) * 2 * k64] = bottom
        else:
            far_left[:half_rows, :] = top
            far_left[half_rows:, :] = bottom

    for slot, shard in enumerate(shards):
        for one in pieces(shard, near_pair.at[0], near_free.at[0], 0, 0, slot):
            one.wait()

    tile = 8
    rows = tile * c
    blocks = near_pair.shape[1]

    def one_block(ib, carry):
        at = pl.multiple_of(ib * rows, rows)
        pair_lhs = near_left[pl.ds(at, rows), :]
        meets = block_meets(where_ref, ib, tile, cols)

        def pair_dot(mp):
            rhs = jnp.concatenate([near_pair[q, mp] for q in range(near)], axis=0)
            return jnp.dot(pair_lhs, rhs, preferred_element_type=F32)

        @pl.when(meets)
        def _():
            lhs = jnp.concatenate(
                [ref[q, pl.ds(half_rows + at, rows), :] for q in range(near) for ref in (mine_ref, theirs_ref)], axis=1
            )
            mask = block_mask(same_scr, ib, tile, c)
            for mp in range(blocks):
                rhs = jnp.concatenate([near_free[q, mp] for q in range(near)], axis=0)
                free = jnp.dot(lhs, rhs, preferred_element_type=F32)
                sum_ref[mp, pl.ds(at, rows), :] = pair_dot(mp) + free * mask

        @pl.when(jnp.logical_not(meets))
        def _():
            for mp in range(blocks):
                sum_ref[mp, pl.ds(at, rows), :] = pair_dot(mp)

        return carry

    lax.fori_loop(0, here // tile, one_block, 0)


def late_kernel(*refs):
    (where_ref, bias_ref, weight_ref, mine_ref, theirs_ref, sum_ref, far_left, _, _, own_ref, par_ref) = refs[:11]
    out_ref, far_pair, far_free, x_scr, same_scr, inv_scr, sems = refs[11:]
    here, cols, z = out_ref.shape
    quarters = mine_ref.shape[0]
    c = mine_ref.shape[1] // (here + here // 2)
    half_rows = here // 2 * c
    sp = far_pair.shape[1] // (2 * quarters)
    sf = far_free.shape[1] // (2 * quarters)
    at = lax.rem(where_ref[3], quarters)
    copies = []
    for which, shard in enumerate((own_ref, par_ref)):
        block = which * quarters + at
        for src, dst in (
            (shard.at[:, :sp, :], far_pair.at[:, pl.ds(pl.multiple_of(block * sp, sp), sp), :]),
            (shard.at[:, sp:, :], far_free.at[:, pl.ds(pl.multiple_of(block * sf, sf), sf), :]),
        ):
            copies.append(pltpu.make_async_copy(src, dst, sems.at[len(copies)]))
            copies[-1].start()
    same, row_chain = same_chain(where_ref, same_scr.shape, cols)
    same_scr[...] = same
    inv_scr[...] = 1.0 / (S_P + same * depth_at(row_chain, where_ref).astype(F32))
    weights = weight_ref[...]
    bias = bias_ref[...]
    for one in copies:
        one.wait()

    tile = 8
    rows = tile * c
    blocks = far_pair.shape[0]
    width = 2 * cols
    last = quarters - 1

    def store_x(result, mp, slot):
        for i in range(tile):
            for t in range(2):
                x_scr[
                    slot * (tile // 2) + i // 2, (mp * 2 + t) * c : (mp * 2 + t + 1) * c, (i % 2) * width : (i % 2 + 1) * width
                ] = result[i * c : (i + 1) * c, t * width : (t + 1) * width].astype(BF16)

    low = lax.broadcasted_iota(jnp.int32, (z, width), 1) < cols

    def one_block(ib, slot, masked):
        at = pl.multiple_of(ib * rows, rows)
        pair_lhs = far_left[pl.ds(at, rows), :]
        if masked:
            lhs = jnp.concatenate([ref[last, pl.ds(half_rows + at, rows), :] for ref in (mine_ref, theirs_ref)], axis=1)
            mask = block_mask(same_scr, ib, tile, c)
        for mp in range(blocks):
            found = jnp.dot(pair_lhs, far_pair[mp], preferred_element_type=F32) + sum_ref[mp, pl.ds(at, rows), :]
            if masked:
                found = found + jnp.dot(lhs, far_free[mp], preferred_element_type=F32) * mask
            store_x(found, mp, slot)
        inv = inv_scr[pl.ds(pl.multiple_of(ib * tile, tile), tile), :width]
        for pair_of in range(tile // 2):
            d = jnp.dot(weights, x_scr[slot * (tile // 2) + pair_of], preferred_element_type=F32)
            for i in range(2):
                lanes = slice(i * width, (i + 1) * width)
                picked = jnp.where(low, d[:z, lanes], d[z:, lanes])
                row = pair_of * 2 + i
                turned = (picked * inv[row : row + 1]).T
                out_ref[ib * tile + row] = (turned[:cols] + turned[cols:] + bias).astype(BF16)

    def all_blocks(masked):
        def some(step, carry):
            for slot in range(TOGETHER):
                one_block(step * TOGETHER + slot, slot, masked)
            return carry

        lax.fori_loop(0, here // tile // TOGETHER, some, 0)

    meets = block_meets(where_ref, 0, here, cols)

    @pl.when(meets)
    def _():
        all_blocks(True)

    @pl.when(jnp.logical_not(meets))
    def _():
        all_blocks(False)


def pack_kernel(where_ref, *refs):
    *parts, out_ref, sems = refs
    count = len(parts)
    me, my_quarter = where_ref[5], where_ref[6]
    copies = []
    for k, part in enumerate(parts):
        to = quarter_at(lax.rem(me + count - k, count), my_quarter)
        copies.append(pltpu.make_async_copy(part, out_ref.at[to], sems.at[k]))
        copies[-1].start()
    for one in copies:
        one.wait()


def body(
    paired_left,
    paired_right,
    unpaired_left,
    unpaired_right,
    out_weight,
    out_bias,
    chain_lengths,
    unpaired_depths,
):
    sp, c, cols = paired_right.shape
    sf = unpaired_right.shape[0]
    here = paired_left.shape[2]
    row_parts, col_parts = lax.axis_size("row"), lax.axis_size("col")
    seq, row, col = lax.axis_index("seq"), lax.axis_index("row"), lax.axis_index("col")
    half_cols = cols // 2
    z = out_weight.shape[1]
    left_sp, left_sf = paired_left.shape[0], unpaired_left.shape[0]
    where = jnp.stack(
        [
            seq,
            row * here,
            (seq * col_parts + col) * left_sf,
            row,
            col * cols + seq * half_cols,
            col,
            row // (row_parts // col_parts),
        ]
    ).astype(jnp.int32)
    where = jnp.concatenate([where, chain_lengths, unpaired_depths])

    shard_shape = jax.ShapeDtypeStruct((c // 4, sp + sf, 2 * cols), BF16)
    own, other = pl.pallas_call(
        right_kernel,
        out_shape=(shard_shape, shard_shape),
        in_specs=[smem(), hbm(), hbm()],
        out_specs=(vmem(), vmem()),
        scratch_shapes=[
            VM(paired_right.shape, BF16),
            VM(unpaired_right.shape, BF16),
            pltpu.SemaphoreType.DMA((2,)),
            VM((sp * c, cols), F32),
            VM((sf * c, cols), F32),
        ],
        compiler_params=limit(6),
    )(where, paired_right, unpaired_right)
    swap = [(0, 1), (1, 0)]
    partner = lax.ppermute(other, "seq", swap)
    up = [(i, (i + 1) % row_parts) for i in range(row_parts)]
    down = [(i, (i - 1) % row_parts) for i in range(row_parts)]
    steps = row_parts // 2
    tied = lax.optimization_barrier
    send = lambda pair: (lax.ppermute(pair[0], "row", up), lax.ppermute(pair[1], "row", down))
    shift = lambda x, k: lax.ppermute(x, "col", [(i, (i + k) % col_parts) for i in range(col_parts)])

    def after(values, *earlier):
        return tied((*values, *earlier))[: len(values)]

    own_ring, par_ring = [own], [partner]
    own_at = send((own, own))
    par_at = send((partner, partner))
    own_ring += own_at
    par_ring += par_at
    paired_left, unpaired_left, out_weight = after((paired_left, unpaired_left, out_weight), own_at[0])
    left, weight = pl.pallas_call(
        left_kernel,
        out_shape=(
            jax.ShapeDtypeStruct((here * c * 3 // 2, left_sf), BF16),
            jax.ShapeDtypeStruct((2 * z, c * c // 2), BF16),
        ),
        in_specs=[smem(), hbm(), hbm(), hbm()],
        out_specs=(vmem(), vmem()),
        scratch_shapes=[
            VM((c, here, left_sp), BF16),
            VM((c, here, left_sf), BF16),
            VM(out_weight.shape, BF16),
            pltpu.SemaphoreType.DMA((3,)),
            VM((c * here, left_sp), F32),
            VM((c * here, left_sf), F32),
            VM((here, left_sf), F32),
            VM((c * c, z), F32),
            VM((c * c // 2, z), F32),
        ],
        compiler_params=limit(10),
    )(
        where,
        jnp.transpose(paired_left, (1, 2, 0)),
        jnp.transpose(unpaired_left, (1, 2, 0)),
        out_weight,
    )
    left_parts = [left]
    for k in range(2, steps + 1):
        before = [par_ring[-3] if k > 2 else partner]
        if k == 3:
            before.append(left)
        if 3 < k <= 3 + col_parts - 1:
            before.append(left_parts[k - 3])
        if k == PACK_STEP + 2:
            before.append(mine)
        own_at = after(own_at, *before)
        par_at = after(par_at, own_ring[-1])
        if k < steps:
            own_at, par_at = send(own_at), send(par_at)
        else:
            own_at, par_at = send(own_at)[:1], send(par_at)[1:]
        own_ring += own_at
        par_ring += par_at
        if k < 2 + col_parts - 1:
            left_parts.append(shift(after((left,), par_ring[2 * k - 3])[0], k - 1))
        if k == PACK_STEP:
            mine = pl.pallas_call(
                pack_kernel,
                out_shape=jax.ShapeDtypeStruct((col_parts, *left.shape), BF16),
                in_specs=[smem()] + [vmem()] * col_parts,
                out_specs=vmem(),
                scratch_shapes=[pltpu.SemaphoreType.DMA((col_parts,))],
                compiler_params=limit(2),
            )(where, *after(left_parts, own_ring[-3]))
            theirs = lax.ppermute(mine, "seq", swap)
    rings = own_ring[:-1] + par_ring[:-1]
    wide = 2 * cols
    pair_rows, free_rows = 2 * left_sp, 2 * left_sf
    blocks = c // 4
    near = col_parts - 1
    total, far_left, far_pair, far_free = pl.pallas_call(
        functools.partial(early_kernel, steps, half_cols),
        out_shape=(
            jax.ShapeDtypeStruct((blocks, here * c, wide), F32),
            jax.ShapeDtypeStruct((here * c, pair_rows), BF16),
            jax.ShapeDtypeStruct((blocks, pair_rows, wide), BF16),
            jax.ShapeDtypeStruct((blocks, free_rows, wide), BF16),
        ),
        in_specs=[smem()] + [vmem()] * (2 + len(rings)),
        out_specs=(vmem(),) * 4,
        scratch_shapes=[
            VM((here * c, near * pair_rows), BF16),
            VM((near, blocks, pair_rows, wide), BF16),
            VM((near, blocks, free_rows, wide), BF16),
            VM((here, wide), F32),
            pltpu.SemaphoreType.DMA((2 * len(rings),)),
        ],
        compiler_params=limit(20),
    )(where, mine, theirs, *rings)
    result, _, _ = pl.pallas_call(
        late_kernel,
        out_shape=(
            jax.ShapeDtypeStruct((here, half_cols, z), BF16),
            jax.ShapeDtypeStruct(far_pair.shape, BF16),
            jax.ShapeDtypeStruct(far_free.shape, BF16),
        ),
        in_specs=[smem()] + [vmem()] * 10,
        out_specs=(vmem(),) * 3,
        input_output_aliases={7: 1, 8: 2},
        scratch_shapes=[
            VM((4 * TOGETHER, c * c // 2, wide), BF16),
            VM((here, wide), F32),
            VM((here, wide), F32),
            pltpu.SemaphoreType.DMA((4,)),
        ],
        compiler_params=limit(16),
    )(where, out_bias.reshape(1, z), weight, mine, theirs, total, far_left, far_pair, far_free, own_ring[-1], par_ring[-1])
    return result


def solution(mesh):
    return jax.shard_map(
        body,
        mesh=mesh,
        in_specs=(
            P(("groups", "seq", "col"), None, "row"),
            P(("groups", "seq", "row"), None, "col"),
            P(("groups", "seq", "col"), None, "row"),
            P(("groups", "seq", "row"), None, "col"),
            P(),
            P(),
            P("groups"),
            P("groups"),
        ),
        out_specs=P(("groups", "row"), ("col", "seq"), None),
        check_vma=False,
    )
```

```python
import functools

import jax
import jax.numpy as jnp
from jax import lax
from jax.experimental import pallas as pl
from jax.experimental.pallas import tpu as pltpu
from jax.sharding import PartitionSpec as P

S_P = 512
F32 = jnp.float32
BF16 = jnp.bfloat16
VM = pltpu.VMEM
SM = pltpu.SMEM


def vmem():
    return pl.BlockSpec(memory_space=VM)


def smem():
    return pl.BlockSpec(memory_space=SM)


def hbm():
    return pl.BlockSpec(memory_space=pl.ANY)


def limit(mib):
    return pltpu.CompilerParams(vmem_limit_bytes=mib * 1024 * 1024)


SCALARS = 7
PACK_STEP = 6
TOGETHER = 2


def chain_count(where_ref):
    return (where_ref.shape[0] - SCALARS) // 2


def chain_ends(where_ref):
    ends, total = [], jnp.int32(0)
    for k in range(chain_count(where_ref)):
        total = total + where_ref[SCALARS + k]
        ends.append(total)
    return ends


def chain_at(ends, position):
    found = (position >= ends[0]).astype(jnp.int32)
    for end in ends[1:]:
        found = found + (position >= end).astype(jnp.int32)
    return found


def depth_at(chain, where_ref):
    depth = jnp.zeros_like(chain)
    chains = chain_count(where_ref)
    for k in range(chains):
        depth = jnp.where(chain == k, where_ref[SCALARS + chains + k], depth)
    return depth


def fetch(sems, *pairs):
    copies = [pltpu.make_async_copy(src, dst, sems.at[k]) for k, (src, dst) in enumerate(pairs)]
    for one in copies:
        one.start()
    for one in copies:
        one.wait()


def right_kernel(pair_hbm, free_hbm, own_ref, other_ref, pair_ref, free_ref, sems, pair_scr, free_scr):
    fetch(sems, (pair_hbm, pair_ref), (free_hbm, free_ref))
    sp, c, cols = pair_ref.shape
    sf = free_ref.shape[0]
    pair_scr[...] = pair_ref[...].astype(F32).reshape(sp * c, cols)
    free_scr[...] = free_ref[...].astype(F32).reshape(sf * c, cols)
    first = lax.axis_index("seq") == 0
    half = cols // 2
    for scr, rows, at in ((pair_scr, sp, 0), (free_scr, sf, sp)):
        lane = lax.broadcasted_iota(jnp.int32, (rows, cols), 1)
        low = lane < half
        for m in range(c // 2):
            lo = scr[pl.ds(m, rows, stride=c), :]
            hi = scr[pl.ds(m + c // 2, rows, stride=c), :]
            zero = jnp.where(low, lo, pltpu.roll(hi, half, 1)).astype(BF16)
            one = jnp.where(low, pltpu.roll(lo, half, 1), hi).astype(BF16)
            mp, t = m % (c // 4), m // (c // 4)
            lanes = slice(t * cols, (t + 1) * cols)
            own_ref[mp, at : at + rows, lanes] = jnp.where(first, zero, one)
            other_ref[mp, at : at + rows, lanes] = jnp.where(first, one, zero)


def left_kernel(
    where_ref, pair_hbm, free_hbm, weight_hbm, out_ref, turned_ref, pair_ref, free_ref, weight_ref, sems, *scratch
):
    pair_scr, free_scr, live_scr, weight_scr, sorted_scr = scratch
    fetch(sems, (weight_hbm, weight_ref), (pair_hbm, pair_ref), (free_hbm, free_ref))
    c, here, sp = pair_ref.shape
    weight_scr[...] = weight_ref[...].astype(F32)
    z = weight_ref.shape[1]
    for b in range(2):
        for m in range(c // 2):
            at = ((m % (c // 4)) * 2 + m // (c // 4)) * c
            sorted_scr[at : at + c, :] = weight_scr[pl.ds(m + b * c // 2, c, stride=c), :]
        turned_ref[b * z : (b + 1) * z, :] = sorted_scr[...].T.astype(BF16)
    sf = free_ref.shape[2]
    pair_scr[...] = pair_ref[...].astype(F32).reshape(c * here, sp)
    free_scr[...] = free_ref[...].astype(F32).reshape(c * here, sf)
    ends = chain_ends(where_ref)
    position = where_ref[1] + lax.broadcasted_iota(jnp.int32, (here, sf), 0)
    depth = depth_at(chain_at(ends, position), where_ref)
    row = where_ref[2] + lax.broadcasted_iota(jnp.int32, (here, sf), 1)
    live_scr[...] = (row < depth).astype(F32)
    for i in range(here // 2):
        a = pair_scr[pl.ds(i, c, stride=here), :]
        b = pair_scr[pl.ds(i + here // 2, c, stride=here), :]
        rows = jnp.concatenate([a, b], axis=1).astype(BF16)
        out_ref[i * c : (i + 1) * c, :] = rows
    base = here * c // 2
    for i in range(here):
        rows = (free_scr[pl.ds(i, c, stride=here), :] * live_scr[i : i + 1, :]).astype(BF16)
        out_ref[base + i * c : base + (i + 1) * c, :] = rows


def quarter_at(quarter, mine):
    step = lax.rem(quarter - mine + 4, 4)
    return jnp.where(step == 2, 3, jnp.where(step == 3, 2, step))


def same_chain(where_ref, shape, cols):
    ends = chain_ends(where_ref)
    lane = lax.rem(lax.broadcasted_iota(jnp.int32, shape, 1), cols)
    row_chain = chain_at(ends, where_ref[1] + lax.broadcasted_iota(jnp.int32, shape, 0))
    same = (row_chain == chain_at(ends, where_ref[4] + lane)).astype(F32)
    return same, row_chain


def block_meets(where_ref, ib, tile, cols):
    ends = chain_ends(where_ref)
    first_row = where_ref[1] + ib * tile
    first_col = where_ref[4]
    return jnp.logical_and(
        chain_at(ends, first_row) <= chain_at(ends, first_col + cols - 1),
        chain_at(ends, first_row + tile - 1) >= chain_at(ends, first_col),
    )


def block_mask(same_scr, ib, tile, c):
    mask = same_scr[pl.ds(pl.multiple_of(ib * tile, tile), tile), :]
    wide = mask.shape[1]
    return jnp.broadcast_to(mask[:, None, :], (tile, c, wide)).reshape(tile * c, wide)


def early_kernel(steps, cols, *refs):
    where_ref, mine_ref, theirs_ref = refs[:3]
    shards = refs[3 : 3 + 2 * (2 * steps - 1)]
    sum_ref, far_left, far_pair, far_free, near_left, near_pair, near_free, same_scr, sems = refs[3 + len(shards) :]
    devices = 2 * steps
    quarters = mine_ref.shape[0]
    per = devices // quarters
    here = same_scr.shape[0]
    c = mine_ref.shape[1] // (here + here // 2)
    me = where_ref[3]
    my_quarter = me // per
    near = quarters - 1

    def place(shard, which, offset, slot):
        source = lax.rem(me + devices + offset, devices)
        to = quarter_at(source // per, my_quarter)
        at = lax.rem(source, per)

        near_at = jnp.minimum(to, near - 1)
        if abs(offset) <= steps - per:
            start(shard, near_pair.at[near_at], near_free.at[near_at], which, at, slot)
            return

        @pl.when(to < near)
        def _():
            start(shard, near_pair.at[near_at], near_free.at[near_at], which, at, slot)

        @pl.when(to == near)
        def _():
            start(shard, far_pair, far_free, which, at, slot)

    def start(shard, pair_dst, free_dst, which, at, slot):
        for one in pieces(shard, pair_dst, free_dst, which, at, slot):
            one.start()

    def pieces(shard, pair_dst, free_dst, which, at, slot):
        sp = pair_dst.shape[1] // (2 * per)
        sf = free_dst.shape[1] // (2 * per)
        block = which * per + at
        return (
            pltpu.make_async_copy(
                shard.at[:, :sp, :], pair_dst.at[:, pl.ds(pl.multiple_of(block * sp, sp), sp), :], sems.at[2 * slot]
            ),
            pltpu.make_async_copy(
                shard.at[:, sp:, :], free_dst.at[:, pl.ds(pl.multiple_of(block * sf, sf), sf), :], sems.at[2 * slot + 1]
            ),
        )

    offsets = [0] + [sign * d for d in range(1, steps) for sign in (-1, 1)]
    for which in range(2):
        for k, offset in enumerate(offsets):
            place(shards[which * len(offsets) + k], which, offset, which * len(offsets) + k)

    same, _ = same_chain(where_ref, same_scr.shape, cols)
    same_scr[...] = same
    half_rows = here // 2 * c
    k64 = mine_ref.shape[2] // 2
    for q in range(quarters):
        a = mine_ref[q, :half_rows, :].astype(F32)
        b = theirs_ref[q, :half_rows, :].astype(F32)
        low = lax.broadcasted_iota(jnp.int32, a.shape, 1) < k64
        top = jnp.where(low, a, pltpu.roll(b, k64, 1)).astype(BF16)
        bottom = jnp.where(low, pltpu.roll(a, k64, 1), b).astype(BF16)
        if q < near:
            near_left[:half_rows, q * 2 * k64 : (q + 1) * 2 * k64] = top
            near_left[half_rows:, q * 2 * k64 : (q + 1) * 2 * k64] = bottom
        else:
            far_left[:half_rows, :] = top
            far_left[half_rows:, :] = bottom

    for slot, shard in enumerate(shards):
        for one in pieces(shard, near_pair.at[0], near_free.at[0], 0, 0, slot):
            one.wait()

    tile = 8
    rows = tile * c
    blocks = near_pair.shape[1]

    def one_block(ib, carry):
        at = pl.multiple_of(ib * rows, rows)
        pair_lhs = near_left[pl.ds(at, rows), :]
        meets = block_meets(where_ref, ib, tile, cols)

        def pair_dot(mp):
            rhs = jnp.concatenate([near_pair[q, mp] for q in range(near)], axis=0)
            return jnp.dot(pair_lhs, rhs, preferred_element_type=F32)

        @pl.when(meets)
        def _():
            lhs = jnp.concatenate(
                [ref[q, pl.ds(half_rows + at, rows), :] for q in range(near) for ref in (mine_ref, theirs_ref)], axis=1
            )
            mask = block_mask(same_scr, ib, tile, c)
            for mp in range(blocks):
                rhs = jnp.concatenate([near_free[q, mp] for q in range(near)], axis=0)
                free = jnp.dot(lhs, rhs, preferred_element_type=F32)
                sum_ref[mp, pl.ds(at, rows), :] = pair_dot(mp) + free * mask

        @pl.when(jnp.logical_not(meets))
        def _():
            for mp in range(blocks):
                sum_ref[mp, pl.ds(at, rows), :] = pair_dot(mp)

        return carry

    lax.fori_loop(0, here // tile, one_block, 0)


def late_kernel(*refs):
    (where_ref, bias_ref, weight_ref, mine_ref, theirs_ref, sum_ref, far_left, _, _, own_ref, par_ref) = refs[:11]
    out_ref, far_pair, far_free, x_scr, same_scr, inv_scr, sems = refs[11:]
    here, cols, z = out_ref.shape
    quarters = mine_ref.shape[0]
    c = mine_ref.shape[1] // (here + here // 2)
    half_rows = here // 2 * c
    sp = far_pair.shape[1] // (2 * quarters)
    sf = far_free.shape[1] // (2 * quarters)
    at = lax.rem(where_ref[3], quarters)
    copies = []
    for which, shard in enumerate((own_ref, par_ref)):
        block = which * quarters + at
        for src, dst in (
            (shard.at[:, :sp, :], far_pair.at[:, pl.ds(pl.multiple_of(block * sp, sp), sp), :]),
            (shard.at[:, sp:, :], far_free.at[:, pl.ds(pl.multiple_of(block * sf, sf), sf), :]),
        ):
            copies.append(pltpu.make_async_copy(src, dst, sems.at[len(copies)]))
            copies[-1].start()
    same, row_chain = same_chain(where_ref, same_scr.shape, cols)
    same_scr[...] = same
    inv_scr[...] = 1.0 / (S_P + same * depth_at(row_chain, where_ref).astype(F32))
    weights = weight_ref[...]
    bias = bias_ref[...]
    for one in copies:
        one.wait()

    tile = 8
    rows = tile * c
    blocks = far_pair.shape[0]
    width = 2 * cols
    last = quarters - 1

    def store_x(result, mp, slot):
        for i in range(tile):
            for t in range(2):
                x_scr[
                    slot * (tile // 2) + i // 2, (mp * 2 + t) * c : (mp * 2 + t + 1) * c, (i % 2) * width : (i % 2 + 1) * width
                ] = result[i * c : (i + 1) * c, t * width : (t + 1) * width].astype(BF16)

    low = lax.broadcasted_iota(jnp.int32, (z, width), 1) < cols

    def one_block(ib, slot, masked):
        at = pl.multiple_of(ib * rows, rows)
        pair_lhs = far_left[pl.ds(at, rows), :]
        if masked:
            lhs = jnp.concatenate([ref[last, pl.ds(half_rows + at, rows), :] for ref in (mine_ref, theirs_ref)], axis=1)
            mask = block_mask(same_scr, ib, tile, c)
        for mp in range(blocks):
            found = jnp.dot(pair_lhs, far_pair[mp], preferred_element_type=F32) + sum_ref[mp, pl.ds(at, rows), :]
            if masked:
                found = found + jnp.dot(lhs, far_free[mp], preferred_element_type=F32) * mask
            store_x(found, mp, slot)
        inv = inv_scr[pl.ds(pl.multiple_of(ib * tile, tile), tile), :width]
        for pair_of in range(tile // 2):
            d = jnp.dot(weights, x_scr[slot * (tile // 2) + pair_of], preferred_element_type=F32)
            for i in range(2):
                lanes = slice(i * width, (i + 1) * width)
                picked = jnp.where(low, d[:z, lanes], d[z:, lanes])
                row = pair_of * 2 + i
                turned = (picked * inv[row : row + 1]).T
                out_ref[ib * tile + row] = (turned[:cols] + turned[cols:] + bias).astype(BF16)

    def all_blocks(masked):
        def some(step, carry):
            for slot in range(TOGETHER):
                one_block(step * TOGETHER + slot, slot, masked)
            return carry

        lax.fori_loop(0, here // tile // TOGETHER, some, 0)

    meets = block_meets(where_ref, 0, here, cols)

    @pl.when(meets)
    def _():
        all_blocks(True)

    @pl.when(jnp.logical_not(meets))
    def _():
        all_blocks(False)


def pack_kernel(where_ref, *refs):
    *parts, out_ref, sems = refs
    count = len(parts)
    me, my_quarter = where_ref[5], where_ref[6]
    copies = []
    for k, part in enumerate(parts):
        to = quarter_at(lax.rem(me + count - k, count), my_quarter)
        copies.append(pltpu.make_async_copy(part, out_ref.at[to], sems.at[k]))
        copies[-1].start()
    for one in copies:
        one.wait()


def body(
    paired_left,
    paired_right,
    unpaired_left,
    unpaired_right,
    out_weight,
    out_bias,
    chain_lengths,
    unpaired_depths,
):
    sp, c, cols = paired_right.shape
    sf = unpaired_right.shape[0]
    here = paired_left.shape[2]
    row_parts, col_parts = lax.axis_size("row"), lax.axis_size("col")
    seq, row, col = lax.axis_index("seq"), lax.axis_index("row"), lax.axis_index("col")
    half_cols = cols // 2
    z = out_weight.shape[1]
    left_sp, left_sf = paired_left.shape[0], unpaired_left.shape[0]
    where = jnp.stack(
        [
            seq,
            row * here,
            (seq * col_parts + col) * left_sf,
            row,
            col * cols + seq * half_cols,
            col,
            row // (row_parts // col_parts),
        ]
    ).astype(jnp.int32)
    where = jnp.concatenate([where, chain_lengths, unpaired_depths])

    shard_shape = jax.ShapeDtypeStruct((c // 4, sp + sf, 2 * cols), BF16)
    own, other = pl.pallas_call(
        right_kernel,
        out_shape=(shard_shape, shard_shape),
        in_specs=[hbm(), hbm()],
        out_specs=(vmem(), vmem()),
        scratch_shapes=[
            VM(paired_right.shape, BF16),
            VM(unpaired_right.shape, BF16),
            pltpu.SemaphoreType.DMA((2,)),
            VM((sp * c, cols), F32),
            VM((sf * c, cols), F32),
        ],
        compiler_params=limit(6),
    )(paired_right, unpaired_right)
    swap = [(0, 1), (1, 0)]
    partner = lax.ppermute(other, "seq", swap)
    up = [(i, (i + 1) % row_parts) for i in range(row_parts)]
    down = [(i, (i - 1) % row_parts) for i in range(row_parts)]
    steps = row_parts // 2
    tied = lax.optimization_barrier
    send = lambda pair: (lax.ppermute(pair[0], "row", up), lax.ppermute(pair[1], "row", down))
    shift = lambda x, k: lax.ppermute(x, "col", [(i, (i + k) % col_parts) for i in range(col_parts)])

    def after(values, *earlier):
        return tied((*values, *earlier))[: len(values)]

    own_ring, par_ring = [own], [partner]
    own_at = send((own, own))
    par_at = send((partner, partner))
    own_ring += own_at
    par_ring += par_at
    paired_left, unpaired_left, out_weight = after((paired_left, unpaired_left, out_weight), own_at[0])
    left, weight = pl.pallas_call(
        left_kernel,
        out_shape=(
            jax.ShapeDtypeStruct((here * c * 3 // 2, left_sf), BF16),
            jax.ShapeDtypeStruct((2 * z, c * c // 2), BF16),
        ),
        in_specs=[smem(), hbm(), hbm(), hbm()],
        out_specs=(vmem(), vmem()),
        scratch_shapes=[
            VM((c, here, left_sp), BF16),
            VM((c, here, left_sf), BF16),
            VM(out_weight.shape, BF16),
            pltpu.SemaphoreType.DMA((3,)),
            VM((c * here, left_sp), F32),
            VM((c * here, left_sf), F32),
            VM((here, left_sf), F32),
            VM((c * c, z), F32),
            VM((c * c // 2, z), F32),
        ],
        compiler_params=limit(10),
    )(
        where,
        jnp.transpose(paired_left, (1, 2, 0)),
        jnp.transpose(unpaired_left, (1, 2, 0)),
        out_weight,
    )
    left_parts = [left]
    for k in range(2, steps + 1):
        before = [par_ring[-3] if k > 2 else partner]
        if k == 3:
            before.append(left)
        if 3 < k <= 3 + col_parts - 1:
            before.append(left_parts[k - 3])
        if k == PACK_STEP + 2:
            before.append(mine)
        own_at = after(own_at, *before)
        par_at = after(par_at, own_ring[-1])
        if k < steps:
            own_at, par_at = send(own_at), send(par_at)
        else:
            own_at, par_at = send(own_at)[:1], send(par_at)[1:]
        own_ring += own_at
        par_ring += par_at
        if k < 2 + col_parts - 1:
            left_parts.append(shift(after((left,), par_ring[2 * k - 3])[0], k - 1))
        if k == PACK_STEP:
            mine = pl.pallas_call(
                pack_kernel,
                out_shape=jax.ShapeDtypeStruct((col_parts, *left.shape), BF16),
                in_specs=[smem()] + [vmem()] * col_parts,
                out_specs=vmem(),
                scratch_shapes=[pltpu.SemaphoreType.DMA((col_parts,))],
                compiler_params=limit(2),
            )(where, *after(left_parts, own_ring[-3]))
            theirs = lax.ppermute(mine, "seq", swap)
    rings = own_ring[:-1] + par_ring[:-1]
    wide = 2 * cols
    pair_rows, free_rows = 2 * left_sp, 2 * left_sf
    blocks = c // 4
    near = col_parts - 1
    total, far_left, far_pair, far_free = pl.pallas_call(
        functools.partial(early_kernel, steps, half_cols),
        out_shape=(
            jax.ShapeDtypeStruct((blocks, here * c, wide), F32),
            jax.ShapeDtypeStruct((here * c, pair_rows), BF16),
            jax.ShapeDtypeStruct((blocks, pair_rows, wide), BF16),
            jax.ShapeDtypeStruct((blocks, free_rows, wide), BF16),
        ),
        in_specs=[smem()] + [vmem()] * (2 + len(rings)),
        out_specs=(vmem(),) * 4,
        scratch_shapes=[
            VM((here * c, near * pair_rows), BF16),
            VM((near, blocks, pair_rows, wide), BF16),
            VM((near, blocks, free_rows, wide), BF16),
            VM((here, wide), F32),
            pltpu.SemaphoreType.DMA((2 * len(rings),)),
        ],
        compiler_params=limit(20),
    )(where, mine, theirs, *rings)
    result, _, _ = pl.pallas_call(
        late_kernel,
        out_shape=(
            jax.ShapeDtypeStruct((here, half_cols, z), BF16),
            jax.ShapeDtypeStruct(far_pair.shape, BF16),
            jax.ShapeDtypeStruct(far_free.shape, BF16),
        ),
        in_specs=[smem()] + [vmem()] * 10,
        out_specs=(vmem(),) * 3,
        input_output_aliases={7: 1, 8: 2},
        scratch_shapes=[
            VM((4 * TOGETHER, c * c // 2, wide), BF16),
            VM((here, wide), F32),
            VM((here, wide), F32),
            pltpu.SemaphoreType.DMA((4,)),
        ],
        compiler_params=limit(16),
    )(where, out_bias.reshape(1, z), weight, mine, theirs, total, far_left, far_pair, far_free, own_ring[-1], par_ring[-1])
    return result


def solution(mesh):
    return jax.shard_map(
        body,
        mesh=mesh,
        in_specs=(
            P(("groups", "seq", "col"), None, "row"),
            P(("groups", "seq", "row"), None, "col"),
            P(("groups", "seq", "col"), None, "row"),
            P(("groups", "seq", "row"), None, "col"),
            P(),
            P(),
            P("groups"),
            P("groups"),
        ),
        out_specs=P(("groups", "row"), ("col", "seq"), None),
        check_vma=False,
    )
```

```python
import functools

import jax
import jax.numpy as jnp
from jax import lax
from jax.experimental import pallas as pl
from jax.experimental.pallas import tpu as pltpu
from jax.sharding import PartitionSpec as P

S_P = 512
F32 = jnp.float32
BF16 = jnp.bfloat16
VM = pltpu.VMEM
SM = pltpu.SMEM


def vmem():
    return pl.BlockSpec(memory_space=VM)


def smem():
    return pl.BlockSpec(memory_space=SM)


def hbm():
    return pl.BlockSpec(memory_space=pl.ANY)


def limit(mib):
    return pltpu.CompilerParams(vmem_limit_bytes=mib * 1024 * 1024)


SCALARS = 7
PACK_STEP = 6
TOGETHER = 2


def chain_count(where_ref):
    return (where_ref.shape[0] - SCALARS) // 2


def chain_ends(where_ref):
    ends, total = [], jnp.int32(0)
    for k in range(chain_count(where_ref)):
        total = total + where_ref[SCALARS + k]
        ends.append(total)
    return ends


def chain_at(ends, position):
    found = (position >= ends[0]).astype(jnp.int32)
    for end in ends[1:]:
        found = found + (position >= end).astype(jnp.int32)
    return found


def depth_at(chain, where_ref):
    depth = jnp.zeros_like(chain)
    chains = chain_count(where_ref)
    for k in range(chains):
        depth = jnp.where(chain == k, where_ref[SCALARS + chains + k], depth)
    return depth


def fetch(sems, *pairs):
    copies = [pltpu.make_async_copy(src, dst, sems.at[k]) for k, (src, dst) in enumerate(pairs)]
    for one in copies:
        one.start()
    for one in copies:
        one.wait()


def right_kernel(pair_ref, free_ref, own_ref, other_ref, pair_scr, free_scr):
    sp, c, cols = pair_ref.shape
    sf = free_ref.shape[0]
    pair_scr[...] = pair_ref[...].astype(F32).reshape(sp * c, cols)
    free_scr[...] = free_ref[...].astype(F32).reshape(sf * c, cols)
    first = lax.axis_index("seq") == 0
    half = cols // 2
    for scr, rows, at in ((pair_scr, sp, 0), (free_scr, sf, sp)):
        lane = lax.broadcasted_iota(jnp.int32, (rows, cols), 1)
        low = lane < half
        for m in range(c // 2):
            lo = scr[pl.ds(m, rows, stride=c), :]
            hi = scr[pl.ds(m + c // 2, rows, stride=c), :]
            zero = jnp.where(low, lo, pltpu.roll(hi, half, 1)).astype(BF16)
            one = jnp.where(low, pltpu.roll(lo, half, 1), hi).astype(BF16)
            mp, t = m % (c // 4), m // (c // 4)
            lanes = slice(t * cols, (t + 1) * cols)
            own_ref[mp, at : at + rows, lanes] = jnp.where(first, zero, one)
            other_ref[mp, at : at + rows, lanes] = jnp.where(first, one, zero)


def left_kernel(
    where_ref, pair_hbm, free_hbm, weight_hbm, out_ref, turned_ref, pair_ref, free_ref, weight_ref, sems, *scratch
):
    pair_scr, free_scr, live_scr, weight_scr, sorted_scr = scratch
    fetch(sems, (weight_hbm, weight_ref), (pair_hbm, pair_ref), (free_hbm, free_ref))
    c, here, sp = pair_ref.shape
    weight_scr[...] = weight_ref[...].astype(F32)
    z = weight_ref.shape[1]
    for b in range(2):
        for m in range(c // 2):
            at = ((m % (c // 4)) * 2 + m // (c // 4)) * c
            sorted_scr[at : at + c, :] = weight_scr[pl.ds(m + b * c // 2, c, stride=c), :]
        turned_ref[b * z : (b + 1) * z, :] = sorted_scr[...].T.astype(BF16)
    sf = free_ref.shape[2]
    pair_scr[...] = pair_ref[...].astype(F32).reshape(c * here, sp)
    free_scr[...] = free_ref[...].astype(F32).reshape(c * here, sf)
    ends = chain_ends(where_ref)
    position = where_ref[1] + lax.broadcasted_iota(jnp.int32, (here, sf), 0)
    depth = depth_at(chain_at(ends, position), where_ref)
    row = where_ref[2] + lax.broadcasted_iota(jnp.int32, (here, sf), 1)
    live_scr[...] = (row < depth).astype(F32)
    for i in range(here // 2):
        a = pair_scr[pl.ds(i, c, stride=here), :]
        b = pair_scr[pl.ds(i + here // 2, c, stride=here), :]
        rows = jnp.concatenate([a, b], axis=1).astype(BF16)
        out_ref[i * c : (i + 1) * c, :] = rows
    base = here * c // 2
    for i in range(here):
        rows = (free_scr[pl.ds(i, c, stride=here), :] * live_scr[i : i + 1, :]).astype(BF16)
        out_ref[base + i * c : base + (i + 1) * c, :] = rows


def quarter_at(quarter, mine):
    step = lax.rem(quarter - mine + 4, 4)
    return jnp.where(step == 2, 3, jnp.where(step == 3, 2, step))


def same_chain(where_ref, shape, cols):
    ends = chain_ends(where_ref)
    lane = lax.rem(lax.broadcasted_iota(jnp.int32, shape, 1), cols)
    row_chain = chain_at(ends, where_ref[1] + lax.broadcasted_iota(jnp.int32, shape, 0))
    same = (row_chain == chain_at(ends, where_ref[4] + lane)).astype(F32)
    return same, row_chain


def block_meets(where_ref, ib, tile, cols):
    ends = chain_ends(where_ref)
    first_row = where_ref[1] + ib * tile
    first_col = where_ref[4]
    return jnp.logical_and(
        chain_at(ends, first_row) <= chain_at(ends, first_col + cols - 1),
        chain_at(ends, first_row + tile - 1) >= chain_at(ends, first_col),
    )


def block_mask(same_scr, ib, tile, c):
    mask = same_scr[pl.ds(pl.multiple_of(ib * tile, tile), tile), :]
    wide = mask.shape[1]
    return jnp.broadcast_to(mask[:, None, :], (tile, c, wide)).reshape(tile * c, wide)


def early_kernel(steps, cols, *refs):
    where_ref, mine_ref, theirs_ref = refs[:3]
    shards = refs[3 : 3 + 2 * (2 * steps - 1)]
    sum_ref, far_left, far_pair, far_free, near_left, near_pair, near_free, same_scr, sems = refs[3 + len(shards) :]
    devices = 2 * steps
    quarters = mine_ref.shape[0]
    per = devices // quarters
    here = same_scr.shape[0]
    c = mine_ref.shape[1] // (here + here // 2)
    me = where_ref[3]
    my_quarter = me // per
    near = quarters - 1

    def place(shard, which, offset, slot):
        source = lax.rem(me + devices + offset, devices)
        to = quarter_at(source // per, my_quarter)
        at = lax.rem(source, per)

        near_at = jnp.minimum(to, near - 1)
        if abs(offset) <= steps - per:
            start(shard, near_pair.at[near_at], near_free.at[near_at], which, at, slot)
            return

        @pl.when(to < near)
        def _():
            start(shard, near_pair.at[near_at], near_free.at[near_at], which, at, slot)

        @pl.when(to == near)
        def _():
            start(shard, far_pair, far_free, which, at, slot)

    def start(shard, pair_dst, free_dst, which, at, slot):
        for one in pieces(shard, pair_dst, free_dst, which, at, slot):
            one.start()

    def pieces(shard, pair_dst, free_dst, which, at, slot):
        sp = pair_dst.shape[1] // (2 * per)
        sf = free_dst.shape[1] // (2 * per)
        block = which * per + at
        return (
            pltpu.make_async_copy(
                shard.at[:, :sp, :], pair_dst.at[:, pl.ds(pl.multiple_of(block * sp, sp), sp), :], sems.at[2 * slot]
            ),
            pltpu.make_async_copy(
                shard.at[:, sp:, :], free_dst.at[:, pl.ds(pl.multiple_of(block * sf, sf), sf), :], sems.at[2 * slot + 1]
            ),
        )

    offsets = [0] + [sign * d for d in range(1, steps) for sign in (-1, 1)]
    for which in range(2):
        for k, offset in enumerate(offsets):
            place(shards[which * len(offsets) + k], which, offset, which * len(offsets) + k)

    same, _ = same_chain(where_ref, same_scr.shape, cols)
    same_scr[...] = same
    half_rows = here // 2 * c
    k64 = mine_ref.shape[2] // 2
    for q in range(quarters):
        a = mine_ref[q, :half_rows, :].astype(F32)
        b = theirs_ref[q, :half_rows, :].astype(F32)
        low = lax.broadcasted_iota(jnp.int32, a.shape, 1) < k64
        top = jnp.where(low, a, pltpu.roll(b, k64, 1)).astype(BF16)
        bottom = jnp.where(low, pltpu.roll(a, k64, 1), b).astype(BF16)
        if q < near:
            near_left[:half_rows, q * 2 * k64 : (q + 1) * 2 * k64] = top
            near_left[half_rows:, q * 2 * k64 : (q + 1) * 2 * k64] = bottom
        else:
            far_left[:half_rows, :] = top
            far_left[half_rows:, :] = bottom

    for slot, shard in enumerate(shards):
        for one in pieces(shard, near_pair.at[0], near_free.at[0], 0, 0, slot):
            one.wait()

    tile = 8
    rows = tile * c
    blocks = near_pair.shape[1]

    def one_block(ib, carry):
        at = pl.multiple_of(ib * rows, rows)
        pair_lhs = near_left[pl.ds(at, rows), :]
        meets = block_meets(where_ref, ib, tile, cols)

        def pair_dot(mp):
            rhs = jnp.concatenate([near_pair[q, mp] for q in range(near)], axis=0)
            return jnp.dot(pair_lhs, rhs, preferred_element_type=F32)

        @pl.when(meets)
        def _():
            lhs = jnp.concatenate(
                [ref[q, pl.ds(half_rows + at, rows), :] for q in range(near) for ref in (mine_ref, theirs_ref)], axis=1
            )
            mask = block_mask(same_scr, ib, tile, c)
            for mp in range(blocks):
                rhs = jnp.concatenate([near_free[q, mp] for q in range(near)], axis=0)
                free = jnp.dot(lhs, rhs, preferred_element_type=F32)
                sum_ref[mp, pl.ds(at, rows), :] = pair_dot(mp) + free * mask

        @pl.when(jnp.logical_not(meets))
        def _():
            for mp in range(blocks):
                sum_ref[mp, pl.ds(at, rows), :] = pair_dot(mp)

        return carry

    lax.fori_loop(0, here // tile, one_block, 0)


def late_kernel(*refs):
    (where_ref, bias_ref, weight_ref, mine_ref, theirs_ref, sum_ref, far_left, _, _, own_ref, par_ref) = refs[:11]
    out_ref, far_pair, far_free, x_scr, same_scr, inv_scr, sems = refs[11:]
    here, cols, z = out_ref.shape
    quarters = mine_ref.shape[0]
    c = mine_ref.shape[1] // (here + here // 2)
    half_rows = here // 2 * c
    sp = far_pair.shape[1] // (2 * quarters)
    sf = far_free.shape[1] // (2 * quarters)
    at = lax.rem(where_ref[3], quarters)
    copies = []
    for which, shard in enumerate((own_ref, par_ref)):
        block = which * quarters + at
        for src, dst in (
            (shard.at[:, :sp, :], far_pair.at[:, pl.ds(pl.multiple_of(block * sp, sp), sp), :]),
            (shard.at[:, sp:, :], far_free.at[:, pl.ds(pl.multiple_of(block * sf, sf), sf), :]),
        ):
            copies.append(pltpu.make_async_copy(src, dst, sems.at[len(copies)]))
            copies[-1].start()
    same, row_chain = same_chain(where_ref, same_scr.shape, cols)
    same_scr[...] = same
    inv_scr[...] = 1.0 / (S_P + same * depth_at(row_chain, where_ref).astype(F32))
    weights = weight_ref[...]
    bias = bias_ref[...]
    for one in copies:
        one.wait()

    tile = 8
    rows = tile * c
    blocks = far_pair.shape[0]
    width = 2 * cols
    last = quarters - 1

    def store_x(result, mp, slot):
        for i in range(tile):
            for t in range(2):
                x_scr[
                    slot * (tile // 2) + i // 2, (mp * 2 + t) * c : (mp * 2 + t + 1) * c, (i % 2) * width : (i % 2 + 1) * width
                ] = result[i * c : (i + 1) * c, t * width : (t + 1) * width].astype(BF16)

    low = lax.broadcasted_iota(jnp.int32, (z, width), 1) < cols

    def one_block(ib, slot, masked):
        at = pl.multiple_of(ib * rows, rows)
        pair_lhs = far_left[pl.ds(at, rows), :]
        if masked:
            lhs = jnp.concatenate([ref[last, pl.ds(half_rows + at, rows), :] for ref in (mine_ref, theirs_ref)], axis=1)
            mask = block_mask(same_scr, ib, tile, c)
        for mp in range(blocks):
            found = jnp.dot(pair_lhs, far_pair[mp], preferred_element_type=F32) + sum_ref[mp, pl.ds(at, rows), :]
            if masked:
                found = found + jnp.dot(lhs, far_free[mp], preferred_element_type=F32) * mask
            store_x(found, mp, slot)
        inv = inv_scr[pl.ds(pl.multiple_of(ib * tile, tile), tile), :width]
        for pair_of in range(tile // 2):
            d = jnp.dot(weights, x_scr[slot * (tile // 2) + pair_of], preferred_element_type=F32)
            for i in range(2):
                lanes = slice(i * width, (i + 1) * width)
                picked = jnp.where(low, d[:z, lanes], d[z:, lanes])
                row = pair_of * 2 + i
                turned = (picked * inv[row : row + 1]).T
                out_ref[ib * tile + row] = (turned[:cols] + turned[cols:] + bias).astype(BF16)

    def all_blocks(masked):
        def some(step, carry):
            for slot in range(TOGETHER):
                one_block(step * TOGETHER + slot, slot, masked)
            return carry

        lax.fori_loop(0, here // tile // TOGETHER, some, 0)

    meets = block_meets(where_ref, 0, here, cols)

    @pl.when(meets)
    def _():
        all_blocks(True)

    @pl.when(jnp.logical_not(meets))
    def _():
        all_blocks(False)


def pack_kernel(where_ref, *refs):
    *parts, out_ref, sems = refs
    count = len(parts)
    me, my_quarter = where_ref[5], where_ref[6]
    copies = []
    for k, part in enumerate(parts):
        to = quarter_at(lax.rem(me + count - k, count), my_quarter)
        copies.append(pltpu.make_async_copy(part, out_ref.at[to], sems.at[k]))
        copies[-1].start()
    for one in copies:
        one.wait()


def body(
    paired_left,
    paired_right,
    unpaired_left,
    unpaired_right,
    out_weight,
    out_bias,
    chain_lengths,
    unpaired_depths,
):
    sp, c, cols = paired_right.shape
    sf = unpaired_right.shape[0]
    here = paired_left.shape[2]
    row_parts, col_parts = lax.axis_size("row"), lax.axis_size("col")
    seq, row, col = lax.axis_index("seq"), lax.axis_index("row"), lax.axis_index("col")
    half_cols = cols // 2
    z = out_weight.shape[1]
    left_sp, left_sf = paired_left.shape[0], unpaired_left.shape[0]
    where = jnp.stack(
        [
            seq,
            row * here,
            (seq * col_parts + col) * left_sf,
            row,
            col * cols + seq * half_cols,
            col,
            row // (row_parts // col_parts),
        ]
    ).astype(jnp.int32)
    where = jnp.concatenate([where, chain_lengths, unpaired_depths])

    shard_shape = jax.ShapeDtypeStruct((c // 4, sp + sf, 2 * cols), BF16)
    own, other = pl.pallas_call(
        right_kernel,
        out_shape=(shard_shape, shard_shape),
        in_specs=[vmem(), vmem()],
        out_specs=(vmem(), vmem()),
        scratch_shapes=[
            VM((sp * c, cols), F32),
            VM((sf * c, cols), F32),
        ],
        compiler_params=limit(6),
    )(paired_right, unpaired_right)
    swap = [(0, 1), (1, 0)]
    partner = lax.ppermute(other, "seq", swap)
    up = [(i, (i + 1) % row_parts) for i in range(row_parts)]
    down = [(i, (i - 1) % row_parts) for i in range(row_parts)]
    steps = row_parts // 2
    tied = lax.optimization_barrier
    send = lambda pair: (lax.ppermute(pair[0], "row", up), lax.ppermute(pair[1], "row", down))
    shift = lambda x, k: lax.ppermute(x, "col", [(i, (i + k) % col_parts) for i in range(col_parts)])

    def after(values, *earlier):
        return tied((*values, *earlier))[: len(values)]

    own_ring, par_ring = [own], [partner]
    own_at = send((own, own))
    par_at = send((partner, partner))
    own_ring += own_at
    par_ring += par_at
    paired_left, unpaired_left, out_weight = after((paired_left, unpaired_left, out_weight), own_at[0])
    left, weight = pl.pallas_call(
        left_kernel,
        out_shape=(
            jax.ShapeDtypeStruct((here * c * 3 // 2, left_sf), BF16),
            jax.ShapeDtypeStruct((2 * z, c * c // 2), BF16),
        ),
        in_specs=[smem(), hbm(), hbm(), hbm()],
        out_specs=(vmem(), vmem()),
        scratch_shapes=[
            VM((c, here, left_sp), BF16),
            VM((c, here, left_sf), BF16),
            VM(out_weight.shape, BF16),
            pltpu.SemaphoreType.DMA((3,)),
            VM((c * here, left_sp), F32),
            VM((c * here, left_sf), F32),
            VM((here, left_sf), F32),
            VM((c * c, z), F32),
            VM((c * c // 2, z), F32),
        ],
        compiler_params=limit(10),
    )(
        where,
        jnp.transpose(paired_left, (1, 2, 0)),
        jnp.transpose(unpaired_left, (1, 2, 0)),
        out_weight,
    )
    left_parts = [left]
    for k in range(2, steps + 1):
        before = [par_ring[-3] if k > 2 else partner]
        if k == 3:
            before.append(left)
        if 3 < k <= 3 + col_parts - 1:
            before.append(left_parts[k - 3])
        if k == PACK_STEP + 2:
            before.append(mine)
        own_at = after(own_at, *before)
        par_at = after(par_at, own_ring[-1])
        if k < steps:
            own_at, par_at = send(own_at), send(par_at)
        else:
            own_at, par_at = send(own_at)[:1], send(par_at)[1:]
        own_ring += own_at
        par_ring += par_at
        if k < 2 + col_parts - 1:
            left_parts.append(shift(after((left,), par_ring[2 * k - 3])[0], k - 1))
        if k == PACK_STEP:
            mine = pl.pallas_call(
                pack_kernel,
                out_shape=jax.ShapeDtypeStruct((col_parts, *left.shape), BF16),
                in_specs=[smem()] + [vmem()] * col_parts,
                out_specs=vmem(),
                scratch_shapes=[pltpu.SemaphoreType.DMA((col_parts,))],
                compiler_params=limit(2),
            )(where, *after(left_parts, own_ring[-3]))
            theirs = lax.ppermute(mine, "seq", swap)
    rings = own_ring[:-1] + par_ring[:-1]
    wide = 2 * cols
    pair_rows, free_rows = 2 * left_sp, 2 * left_sf
    blocks = c // 4
    near = col_parts - 1
    total, far_left, far_pair, far_free = pl.pallas_call(
        functools.partial(early_kernel, steps, half_cols),
        out_shape=(
            jax.ShapeDtypeStruct((blocks, here * c, wide), F32),
            jax.ShapeDtypeStruct((here * c, pair_rows), BF16),
            jax.ShapeDtypeStruct((blocks, pair_rows, wide), BF16),
            jax.ShapeDtypeStruct((blocks, free_rows, wide), BF16),
        ),
        in_specs=[smem()] + [vmem()] * (2 + len(rings)),
        out_specs=(vmem(),) * 4,
        scratch_shapes=[
            VM((here * c, near * pair_rows), BF16),
            VM((near, blocks, pair_rows, wide), BF16),
            VM((near, blocks, free_rows, wide), BF16),
            VM((here, wide), F32),
            pltpu.SemaphoreType.DMA((2 * len(rings),)),
        ],
        compiler_params=limit(20),
    )(where, mine, theirs, *rings)
    result, _, _ = pl.pallas_call(
        late_kernel,
        out_shape=(
            jax.ShapeDtypeStruct((here, half_cols, z), BF16),
            jax.ShapeDtypeStruct(far_pair.shape, BF16),
            jax.ShapeDtypeStruct(far_free.shape, BF16),
        ),
        in_specs=[smem()] + [vmem()] * 10,
        out_specs=(vmem(),) * 3,
        input_output_aliases={7: 1, 8: 2},
        scratch_shapes=[
            VM((4 * TOGETHER, c * c // 2, wide), BF16),
            VM((here, wide), F32),
            VM((here, wide), F32),
            pltpu.SemaphoreType.DMA((4,)),
        ],
        compiler_params=limit(16),
    )(where, out_bias.reshape(1, z), weight, mine, theirs, total, far_left, far_pair, far_free, own_ring[-1], par_ring[-1])
    return result


def solution(mesh):
    return jax.shard_map(
        body,
        mesh=mesh,
        in_specs=(
            P(("groups", "seq", "col"), None, "row"),
            P(("groups", "seq", "row"), None, "col"),
            P(("groups", "seq", "col"), None, "row"),
            P(("groups", "seq", "row"), None, "col"),
            P(),
            P(),
            P("groups"),
            P("groups"),
        ),
        out_specs=P(("groups", "row"), ("col", "seq"), None),
        check_vma=False,
    )
```
